128 devices in a mesh: dp: 16 (over x, y), tensor: 8 (over z, core).
Axes of the slice: x: 4, y: 4, z: 4, core: 2. Of those that a mesh axis runs over, the one named last changes fastest.
Arguments:
- hidden: bfloat16 [4096, 28672], P('dp', 'tensor'), may hold values from -6 to 6
- hidden_check: bfloat16 [16, 28672], P(None, 'tensor'), may hold values from -96 to 96
- down_weight: bfloat16 [28672, 8192], P('tensor', 'dp'), may hold values from -0.03125 to 0.03125
- weight_check: bfloat16 [28672, 64], P('tensor', 'dp'), may hold values from -0.40039062 to 0.40039062
Outputs:
- output: bfloat16 [4096, 8192], P('tensor', 'dp')
- row_residual: float32 [4096, 64], P('tensor', 'dp')
- col_residual: float32 [8192], P('dp')
The draws below stay inside these ranges and needn't reach their ends.
All inputs are finite; a program needn't handle non-finite values.
Results may differ from the reference program's by a relative error of at most 0.001.
Values may be sent and summed in bfloat16 or wider, within the bound.
A program may use at most 128 MiB of HBM per device.

```python
import jax
import jax.numpy as jnp

D = 8192
FF = 28672
CHECK_BLOCK = 128
TOK_DEV = 256
TOKENS = 4096
GROUPS = 16


def shard_levels(rng, dims, shards, least, top_value):
    level = 1.0
    for axis_at, parts in shards:
        heights = jax.random.uniform(jax.random.fold_in(jax.random.fold_in(rng, 6), axis_at), (parts,), jnp.float32, least / len(shards), top_value / len(shards))
        level = level * jnp.repeat(jnp.exp(heights), dims[axis_at] // parts).reshape((-1,) + (1,) * (len(dims) - 1 - axis_at))
    return level


def scatter_about(stream_key, extent, scale, most, pieces=(), held_as=jnp.bfloat16):
    gain = shard_levels(stream_key, extent, pieces, -0.22, 0.18) if pieces else 1.0
    values = jax.random.normal(stream_key, extent, jnp.float32) * scale * gain
    return jnp.minimum(jnp.maximum(values, -most), most).astype(held_as)


def setup_inputs(seed: int = 0) -> dict:
    arg_keys = jax.random.split(jax.random.key(seed), 5)
    return {
        "hidden": scatter_about(arg_keys[0], (TOKENS, FF), 1.0, 6.0, ((0, 16), (1, 8))),
        "hidden_check": scatter_about(arg_keys[1], (GROUPS, FF), (TOK_DEV ** 0.5), 96.0, ((1, 8),)),
        "down_weight": scatter_about(arg_keys[2], (FF, D), FF ** -0.5, 0.03125, ((0, 8), (1, 16))),
        "weight_check": scatter_about(arg_keys[3], (FF, D // CHECK_BLOCK), ((CHECK_BLOCK / FF) ** 0.5), 0.40039062, ((0, 8), (1, 16))),
    }


def reference(hidden, hidden_check, down_weight, weight_check):
    product = jnp.dot(hidden, down_weight, preferred_element_type=jnp.float32)
    output = product.astype(jnp.bfloat16)
    check_cols = jnp.dot(hidden, weight_check, preferred_element_type=jnp.float32)
    rows = product.shape[0]
    block_sums = product.reshape(rows, -1, CHECK_BLOCK).sum(-1)
    row_residual = (check_cols - block_sums) * (CHECK_BLOCK ** -0.5)
    check_rows = jnp.dot(hidden_check, down_weight, preferred_element_type=jnp.float32)
    col_residual = (check_rows.sum(0) - product.sum(0)) * (rows ** -0.5)
    return output, row_residual, col_residual
```

```python
import jax
import jax.numpy as jnp
from jax import lax
from jax.experimental import pallas as pl
from jax.experimental.pallas import tpu as pltpu
from jax.sharding import PartitionSpec as P

CHECK_BLOCK = 128
MESH = pl.DeviceIdType.MESH

PIECE = 64
N_PIECE = 4
ROWS = 72
PIECES = 32


def kernel(
    h_hbm,
    hc_ref,
    w_hbm,
    wc_ref,
    out_hbm,
    rr_ref,
    col_ref,
    hbuf,
    wbuf,
    wcpar,
    wct,
    pbuf,
    rbuf,
    zr,
    obuf,
    rrbuf,
    rrpar,
    cbuf,
    cpar,
    vbuf,
    lsem,
    hs,
    hr,
    ws,
    wr,
    ds_s,
    ds_r,
    zs,
    zrs,
    os_s,
    os_r,
    vs,
    vr,
):
    dp = lax.axis_index("dp")
    t = lax.axis_index("tensor")
    x, y = dp // 4, dp % 4
    z, c = t // 2, t % 2
    group = y // 2
    role = (c + group) % 2
    x_next = ((x + 1) % 4) * 4 + y
    x_prev = ((x + 3) % 4) * 4 + y
    y_near = x * 4 + (y // 2) * 2 + (y + 1) % 2
    y_far = x * 4 + 3 - y
    t_other = z * 2 + 1 - c

    def remote(src, dst, send, recv, dev):
        return pltpu.make_async_remote_copy(
            src_ref=src, dst_ref=dst, send_sem=send, recv_sem=recv, device_id=dev, device_id_type=MESH
        )

    h_in = [
        pltpu.make_async_copy(h_hbm.at[pl.ds(PIECE * i, PIECE)], hbuf.at[pl.ds(PIECE * i, PIECE)], lsem.at[i])
        for i in range(N_PIECE)
    ]
    w_in = [
        pltpu.make_async_copy(w_hbm.at[:, pl.ds(256 * j, 256)], wbuf.at[j], lsem.at[N_PIECE + j]) for j in range(2)
    ]
    for copy in h_in + w_in:
        copy.start()

    barrier = pltpu.get_barrier_semaphore()
    peers = [(x_next, t), (x_prev, t), (y_near, t), (y_far, t), (y_far, t_other)]
    peers += [(dp, (t + d) % 8) for d in range(1, 8)]
    for peer in peers:
        pl.semaphore_signal(barrier, inc=1, device_id=peer, device_id_type=MESH)
    pl.semaphore_wait(barrier, len(peers))

    def step_row(s):
        if s < 4:
            return 256 + 192 * s
        if s < 6:
            return 1024 + 128 * (s - 4)
        return 1280 + 192 * (s - 6)

    def h_copy(s, d):
        if s < 4:
            row = PIECE * s
        elif d == 2:
            k = s - 6
            row = step_row(4 + k // 2) + PIECE * (k % 2)
        elif s < 6:
            row = step_row(s - 4) if d == 0 else step_row(s - 2) + PIECE
        else:
            row = step_row(s - 6) + 2 * PIECE
        dev = ((x_next, t), (x_prev, t), (y_near, t))[d]
        return remote(
            hbuf.at[pl.ds(row, PIECE)], hbuf.at[pl.ds(step_row(s) + PIECE * d, PIECE)], hs.at[s, d], hr.at[s, d], dev
        )

    def dirs(s):
        return (0, 1) if s in (4, 5) else (0, 1, 2)

    for i in range(N_PIECE):
        h_in[i].wait()
        for d in dirs(i):
            h_copy(i, d).start()
    wc_copy = remote(wc_ref, wcpar, ws.at[2], wr.at[2], (y_far, t))
    wc_copy.start()
    w_copy = [remote(wbuf.at[j], wbuf.at[2 + j], ws.at[j], wr.at[j], (y_far, t)) for j in range(2)]
    for j in range(2):
        w_in[j].wait()
        w_copy[j].start()

    def give(j, p):
        @pl.when(j // 2 != role)
        def _():
            remote(
                pbuf.at[j, p], rbuf.at[j % 2, p], ds_s.at[j % 2, p], ds_r.at[j % 2, p], (dp, t_other)
            ).start()

    def mm(row, m, piece, j):
        out = jnp.dot(hbuf[pl.ds(row, m), :], wbuf[j], preferred_element_type=jnp.float32)
        for i in range(m // PIECE):
            pbuf[j, piece + i, 0:PIECE, :] = out[PIECE * i : PIECE * (i + 1)]
        for i in range(m // PIECE):
            give(j, piece + i)

    def checks(row, m, piece):
        out = lax.dot_general(
            hbuf[pl.ds(row, m), :], wct[...], (((1,), (1,)), ((), ())), preferred_element_type=jnp.float32
        )
        for i in range(m // PIECE):
            turned = out[PIECE * i : PIECE * (i + 1)].T
            pbuf[0, piece + i, PIECE:ROWS, 0:PIECE] = turned[0:8]
            pbuf[2, piece + i, PIECE:ROWS, 0:PIECE] = turned[16:24]

    def compute(row, m, piece, n_j):
        checks(row, m, piece)

        @pl.loop(0, n_j)
        def _(j):
            mm(row, m, piece, j)

    def add_up(half, p, zd, q):
        remote(pbuf.at[0, p], rbuf.at[half, p], ds_s.at[half, p], ds_r.at[half, p], (dp, t_other)).wait_recv()
        total = pbuf[2 * role + half, p] + rbuf[half, p]

        @pl.when(zd == z)
        def _():
            zr[z, half, q] = total

        @pl.when(zd != z)
        def _():
            pbuf[2 * role + half, p] = total
            remote(
                pbuf.at[2 * role + half, p],
                zr.at[z, half, q],
                zs.at[half, p],
                zrs.at[z, half, q],
                (dp, zd * 2 + c),
            ).start()

    q_own = (y % 2) * 4
    q_near = ((y + 1) % 2) * 4

    def own_dest(i):
        return i, x, q_own + i

    def a_dest(s, d):
        return 4 + 3 * s + d, (x + (3, 1, 0)[d]) % 4, (q_own, q_own, q_near)[d] + s

    def b_dest(s, d):
        return 16 + 2 * s + d, (x + 2) % 4, q_own + s + 2 * d

    def c_dest(s, d):
        place = s if d < 2 else s // 2 + 2 * (s % 2)
        return 20 + 3 * s + d, (x + (3, 1, 2)[d]) % 4, q_near + place

    def add_own(half):
        @pl.loop(0, 4)
        def _(i):
            p, zd, q = own_dest(i)
            add_up(half, p, zd, q)

    def add_step(dest, n_d, s, half):
        for d in range(n_d):
            p, zd, q = dest(s, d)
            add_up(half, p, zd, q)

    wct[...] = jnp.zeros_like(wct)
    wct[0:4, :] = wc_ref[...]
    wc_copy.wait_recv()
    wct[16:20, :] = wcpar[...]

    compute(0, 256, 0, 2)

    @pl.when(role == 0)
    def _():
        @pl.loop(0, 2)
        def _(half):
            add_own(half)

    for half in range(2):
        rows = jnp.dot(hc_ref[...], wbuf[half], preferred_element_type=jnp.float32)
        cbuf[:, 256 * half : 256 * (half + 1)] = rows[0:8] + rows[8:16]

    def arrive(s):
        for d in dirs(s):
            h_copy(s, d).wait_recv()
        if 4 <= s + 2 < 10:
            for d in dirs(s + 2):
                h_copy(s + 2, d).start()

    def both(n_half, dest, n_d, s):
        @pl.when(role == 0)
        def _():
            @pl.loop(0, 2)
            def _(half):
                add_step(dest, n_d, s, half)

        if n_half:

            @pl.when(role == 1)
            def _():
                @pl.loop(0, n_half)
                def _(half):
                    add_step(dest, n_d, s, half)

    for s in range(10):
        arrive(s)
        if s < 4:
            compute(step_row(s), 192, 4 + 3 * s, 2)
            both(0, a_dest, 3, s)
        elif s < 6:
            compute(step_row(s), 128, 16 + 2 * (s - 4), 3)
            both(1, b_dest, 2, s - 4)
        else:
            compute(step_row(s), 192, 20 + 3 * (s - 6), 3 if s < 8 else 4)
            both(1 if s < 8 else 2, c_dest, 3, s - 6)
        if s == 3:
            w_copy[0].wait_recv()

            @pl.loop(0, 4)
            def _(i):
                mm(256 * i, 256, 4 * i, 2)

            @pl.when(role == 1)
            def _():
                add_own(0)

                @pl.loop(0, 4)
                def _(k):
                    add_step(a_dest, 3, k, 0)

        if s == 7:
            w_copy[1].wait_recv()

            @pl.loop(0, 13)
            def _(i):
                mm(128 * i, 128, 2 * i, 3)

            @pl.when(role == 1)
            def _():
                add_own(1)

                @pl.loop(0, 4)
                def _(k):
                    add_step(a_dest, 3, k, 1)

                @pl.loop(0, 2)
                def _(k):
                    add_step(b_dest, 2, k, 1)
                    add_step(c_dest, 3, k, 1)

    lane = lax.broadcasted_iota(jnp.int32, (PIECE, 128), 1)
    vbuf[t] = jnp.zeros_like(vbuf[t])

    @pl.loop(0, 8)
    def _(q):
        for d in range(1, 4):
            for half in range(2):
                zf = (z + d) % 4
                remote(
                    pbuf.at[0, 0], zr.at[zf, half, q], zs.at[0, 0], zrs.at[zf, half, q], (dp, zf * 2 + c)
                ).wait_recv()
        marks = jnp.zeros((PIECE, 128), jnp.float32)
        for half in range(2):
            full = (zr[0, half, q, 0:PIECE, :] + zr[1, half, q, 0:PIECE, :]) + (
                zr[2, half, q, 0:PIECE, :] + zr[3, half, q, 0:PIECE, :]
            )
            obuf[pl.ds(q * PIECE, PIECE), 256 * half : 256 * (half + 1)] = full.astype(jnp.bfloat16)
            vbuf[t, :, 256 * half : 256 * (half + 1)] += full.reshape(8, 8, 256).sum(0)
            for b in range(2):
                sums = full[:, 128 * b : 128 * (b + 1)].sum(-1, keepdims=True)
                marks = jnp.where(lane == 2 * half + b, sums, marks)
        check = (zr[0, 0, q, PIECE:ROWS, 0:PIECE] + zr[1, 0, q, PIECE:ROWS, 0:PIECE]) + (
            zr[2, 0, q, PIECE:ROWS, 0:PIECE] + zr[3, 0, q, PIECE:ROWS, 0:PIECE]
        )
        rrbuf[q, :, 0:PIECE] = (check - marks.T[0:8]) * CHECK_BLOCK ** (-0.5)

    partner = (y_far, t_other)
    out_far = remote(obuf, out_hbm, os_s.at[0], os_r.at[0], partner)
    rr_far = remote(rrbuf, rrpar, os_s.at[1], os_r.at[1], partner)
    col_far = remote(vbuf.at[t], cpar, os_s.at[2], os_r.at[2], partner)
    out_near = pltpu.make_async_copy(obuf, out_hbm, lsem.at[6])

    def write_rows(src):
        for q in range(8):
            rr_ref[:, PIECE * q : PIECE * (q + 1)] = src[q, 0:4, 0:PIECE]

    @pl.when(role == 0)
    def _():
        out_near.start()
        vbuf[t] = cbuf[...] - vbuf[t]
        write_rows(rrbuf)

    @pl.when(role == 1)
    def _():
        col_far.start()
        rr_far.start()
        out_far.start()
        col_far.wait()
        vbuf[t] = cbuf[...] - cpar[...]

    for d in range(1, 8):
        remote(vbuf.at[t], vbuf.at[t], vs.at[d - 1], vr.at[t], (dp, (t + d) % 8)).start()

    @pl.when(role == 0)
    def _():
        out_near.wait()

    @pl.when(role == 1)
    def _():
        rr_far.wait()
        write_rows(rrpar)
        out_far.wait()

    for d in range(1, 8):
        src = (t + d) % 8
        remote(vbuf.at[src], vbuf.at[src], vs.at[d - 1], vr.at[src], (dp, src)).wait_recv()
    total = vbuf[0]
    for i in range(1, 8):
        total = total + vbuf[i]
    col_ref[...] = total.sum(0, keepdims=True) * 4096 ** (-0.5)

    for d in range(1, 8):
        remote(vbuf.at[t], vbuf.at[t], vs.at[d - 1], vr.at[t], (dp, (t + d) % 8)).wait_send()
    for s in range(10):
        for d in dirs(s):
            h_copy(s, d).wait_send()
    wc_copy.wait_send()
    for j in range(2):
        w_copy[j].wait_send()

    @pl.loop(0, 2)
    def _(half):
        @pl.loop(0, PIECES)
        def _(p):
            remote(
                pbuf.at[0, p], rbuf.at[half, p], ds_s.at[half, p], ds_r.at[half, p], (dp, t_other)
            ).wait_send()

        def sent(p, zd):
            @pl.when(zd != z)
            def _():
                remote(pbuf.at[0, p], zr.at[0, half, 0], zs.at[half, p], zrs.at[z, half, 0], (dp, t_other)).wait_send()

        for i in range(4):
            sent(*own_dest(i)[:2])
            for d in range(3):
                sent(*a_dest(i, d)[:2])
                sent(*c_dest(i, d)[:2])
        for i in range(2):
            for d in range(2):
                sent(*b_dest(i, d)[:2])


def shards(hidden, hidden_check, down_weight, weight_check):
    f32, bf16 = jnp.float32, jnp.bfloat16
    k = hidden.shape[1]
    dma = pltpu.SemaphoreType.DMA
    out, rr, col = pl.pallas_call(
        kernel,
        out_shape=(
            jax.ShapeDtypeStruct((512, 512), bf16),
            jax.ShapeDtypeStruct((4, 512), f32),
            jax.ShapeDtypeStruct((1, 512), f32),
        ),
        in_specs=[
            pl.BlockSpec(memory_space=pl.ANY),
            pl.BlockSpec(memory_space=pltpu.VMEM),
            pl.BlockSpec(memory_space=pl.ANY),
            pl.BlockSpec(memory_space=pltpu.VMEM),
        ],
        out_specs=(
            pl.BlockSpec(memory_space=pl.ANY),
            pl.BlockSpec(memory_space=pltpu.VMEM),
            pl.BlockSpec(memory_space=pltpu.VMEM),
        ),
        scratch_shapes=[
            pltpu.VMEM((2048, k), bf16),
            pltpu.VMEM((4, k, 256), bf16),
            pltpu.VMEM((4, k), bf16),
            pltpu.VMEM((128, k), bf16),
            pltpu.VMEM((4, PIECES, ROWS, 256), f32),
            pltpu.VMEM((2, PIECES, ROWS, 256), f32),
            pltpu.VMEM((4, 2, 8, ROWS, 256), f32),
            pltpu.VMEM((512, 512), bf16),
            pltpu.VMEM((8, 8, 128), f32),
            pltpu.VMEM((8, 8, 128), f32),
            pltpu.VMEM((8, 512), f32),
            pltpu.VMEM((8, 512), f32),
            pltpu.VMEM((8, 8, 512), f32),
            dma((7,)),
            dma((10, 3)),
            dma((10, 3)),
            dma((3,)),
            dma((3,)),
            dma((2, PIECES)),
            dma((2, PIECES)),
            dma((2, PIECES)),
            dma((4, 2, 8)),
            dma((3,)),
            dma((3,)),
            dma((7,)),
            dma((8,)),
        ],
        compiler_params=pltpu.CompilerParams(
            collective_id=0, has_side_effects=True, vmem_limit_bytes=60 * 1024 * 1024
        ),
    )(hidden, hidden_check, down_weight, weight_check.T)
    return out, rr.T, col.reshape(512)


def solution(mesh):
    placed = (P("dp", "tensor"), P(None, "tensor"), P("tensor", "dp"), P("tensor", "dp"))
    return jax.shard_map(
        shards,
        mesh=mesh,
        in_specs=placed,
        out_specs=(P("tensor", "dp"), P("tensor", "dp"), P("dp")),
        check_vma=False,
    )
```

```python
import jax
import jax.numpy as jnp
from jax import lax
from jax.experimental import pallas as pl
from jax.experimental.pallas import tpu as pltpu
from jax.sharding import PartitionSpec as P

CHECK_BLOCK = 128
MESH = pl.DeviceIdType.MESH

PIECE = 32
OWN = 8
STEPS = 19
PIECES = 64
ROWS = (40, 32)


def kernel(
    h_hbm, hc_hbm, w_hbm, wc_hbm,
    out_hbm, rr_ref, col_ref,
    hbuf, wbuf, hcbuf, wcown, wcpar, wct, wck, pbuf, rbuf, rl, zr, obuf, rrbuf, rrt, rrpar, cbuf, cpar, vbuf,
    lsem, osem, hs, hr, ws, wr, ds_s, ds_r, zs, zrs, rls, os_s, os_r, fs, fr, vs, vr,
):
    f32, bf16 = jnp.float32, jnp.bfloat16
    dp = lax.axis_index("dp")
    t = lax.axis_index("tensor")
    x, y = dp // 4, dp % 4
    z, c = t // 2, t % 2
    group = y // 2
    role = (c + group) % 2
    x_next = ((x + 1) % 4) * 4 + y
    x_prev = ((x + 3) % 4) * 4 + y
    y_near = x * 4 + (y // 2) * 2 + (y + 1) % 2
    y_far = x * 4 + 3 - y
    t_other = z * 2 + 1 - c
    partner = (y_far, t_other)

    def remote(src, dst, send, recv, dev):
        return pltpu.make_async_remote_copy(
            src_ref=src, dst_ref=dst, send_sem=send, recv_sem=recv, device_id=dev, device_id_type=MESH
        )

    h_in = pltpu.make_async_copy(h_hbm, hbuf.at[pl.ds(0, PIECE * OWN)], lsem.at[0])
    w_in = [pltpu.make_async_copy(w_hbm.at[:, pl.ds(256 * j, 256)], wbuf.at[j], lsem.at[1 + j]) for j in range(2)]
    hc_in = pltpu.make_async_copy(hc_hbm, hcbuf, lsem.at[3])
    wc_in = pltpu.make_async_copy(wc_hbm, wcown, lsem.at[4])
    h_in.start()
    wc_in.start()
    w_in[0].start()
    w_in[1].start()
    hc_in.start()

    barrier = pltpu.get_barrier_semaphore()
    peers = [(x_next, t), (x_prev, t), (y_near, t), (y_far, t), partner]
    peers += [(dp, (t + d) % 8) for d in range(1, 8)]
    for peer in peers:
        pl.semaphore_signal(barrier, inc=1, device_id=peer, device_id_type=MESH)
    pl.semaphore_wait(barrier, len(peers))

    def piece(s, d):
        return OWN + 3 * s + d

    def source(s, d):
        if s < 8:
            return s
        if d == 2:
            if s < 10:
                return piece(0, s - 8)
            return piece(8 + (s - 10) // 2, (s - 10) % 2)
        if s < 12:
            return piece(s - 8, 0) if d == 0 else piece(s - 4, 1)
        return piece(s - 11, 2)

    def dirs(s):
        return range(3) if s < STEPS - 1 else range(2)

    def h_copy(s, d):
        dev = ((x_next, t), (x_prev, t), (y_near, t))[d]
        return remote(
            hbuf.at[pl.ds(PIECE * source(s, d), PIECE)],
            hbuf.at[pl.ds(PIECE * piece(s, d), PIECE)],
            hs.at[s, d],
            hr.at[s, d],
            dev,
        )

    h_in.wait()
    for s in range(OWN):
        for d in dirs(s):
            h_copy(s, d).start()
    wc_in.wait()
    wc_copy = remote(wcown, wcpar, ws.at[2], wr.at[2], (y_far, t))
    wc_copy.start()
    w_copy = [remote(wbuf.at[j], wbuf.at[2 + j], ws.at[j], wr.at[j], (y_far, t)) for j in range(2)]
    for j in range(2):
        w_in[j].wait()
        w_copy[j].start()

    def core_copy(j, half, p):
        rows = pl.ds(0, ROWS[half])
        return remote(
            pbuf.at[j, p, rows], rbuf.at[half, p, rows], ds_s.at[half, p], ds_r.at[half, p], (dp, t_other)
        )

    def mm(row, m, p, j):
        out = jnp.dot(hbuf[pl.ds(row, m), :], wbuf[j], preferred_element_type=f32)
        for i in range(m // PIECE):
            pbuf[j, p + i, 0:PIECE, :] = out[PIECE * i : PIECE * (i + 1)]
        for half in range(2):

            @pl.when(j == 2 * (1 - role) + half)
            def _():
                for i in range(m // PIECE):
                    core_copy(j, half, p + i).start()

    def checks(row, m, p):
        out = jnp.dot(hbuf[pl.ds(row, m), :], wck[...], preferred_element_type=f32)
        for i in range(m // PIECE):
            turned = out[PIECE * i : PIECE * (i + 1)].T
            pbuf[0, p + i, PIECE : PIECE + 8, 0:PIECE] = turned[0:8]
            pbuf[2, p + i, PIECE : PIECE + 8, 0:PIECE] = turned[16:24]

    def compute(p, n_p, n_j):
        checks(PIECE * p, PIECE * n_p, p)

        @pl.loop(0, n_j)
        def _(i):
            j = (i + 2 * (1 - role)) % 4 if n_j == 4 else i
            mm(PIECE * p, PIECE * n_p, p, j)

    def add_up(half, p, zd, q):
        rows = pl.ds(0, ROWS[half])
        j = 2 * role + half
        core_copy(j, half, p).wait_recv()
        total = pbuf[j, p, 0 : ROWS[half]] + rbuf[half, p, 0 : ROWS[half]]
        away = (zd - z + 4) % 4

        @pl.when(away == 0)
        def _():
            zr[0, half, q, 0 : ROWS[half]] = total

        @pl.when(away != 0)
        def _():
            pbuf[j, p, 0 : ROWS[half]] = total

        @pl.when(away == 2)
        def _():
            to = (z + (1, 3)[half]) % 4
            remote(
                pbuf.at[j, p, rows], rl.at[half, q, rows], zs.at[half, p], rls.at[half, q], (dp, to * 2 + c)
            ).start()

        @pl.when(away == (3, 1)[half])
        def _():
            remote(
                pbuf.at[j, p, rows],
                zr.at[2 - half, half, q, rows],
                zs.at[half, p],
                zrs.at[1 - half, half, q],
                (dp, zd * 2 + c),
            ).start()

    def pass_on(half, p, zd, q):
        rows = pl.ds(0, ROWS[half])
        j = 2 * role + half

        @pl.when((zd - z + 4) % 4 == (1, 3)[half])
        def _():
            remote(pbuf.at[j, p, rows], rl.at[half, q, rows], zs.at[half, p], rls.at[half, q], (dp, t_other)).wait_recv()
            pbuf[j, p, 0 : ROWS[half]] += rl[half, q, 0 : ROWS[half]]
            remote(
                pbuf.at[j, p, rows],
                zr.at[1 + half, half, q, rows],
                zs.at[half, p],
                zrs.at[half, half, q],
                (dp, zd * 2 + c),
            ).start()

    q_own = (y % 2) * OWN
    q_near = ((y + 1) % 2) * OWN

    def own_dest(i):
        return i, x, q_own + i

    def early_dest(s, d):
        return piece(s, d), (x + (3, 1, 0)[d]) % 4, (q_own, q_own, q_near)[d] + s

    def late_dest(s, d):
        if d == 2:
            if s < 10:
                return piece(s, d), (x + (3, 1)[s - 8]) % 4, q_near
            k = s - 10
            return piece(s, d), (x + 2) % 4, q_near + k // 2 + 4 * (k % 2)
        if s < 12:
            return piece(s, d), (x + 2) % 4, q_own + s - (8, 4)[d]
        return piece(s, d), (x + (3, 1)[d]) % 4, q_near + s - 11

    def own_items(half):
        def run(act):
            @pl.loop(0, OWN)
            def _(i):
                act(half, *own_dest(i))

        return run

    def early_items(low, high, half):
        def run(act):
            @pl.loop(low, high)
            def _(s):
                for d in range(3):
                    act(half, *early_dest(s, d))

        return run

    def late_items(low, high, half):
        def run(act):
            for s in range(low, high):
                for d in dirs(s):
                    act(half, *late_dest(s, d))

        return run

    waiting = [[], []]

    def relay():
        for r in range(2):
            if waiting[r]:

                @pl.when(role == r)
                def _():
                    for run in waiting[r]:
                        run(pass_on)

                waiting[r] = []

    def collect(r, items):
        @pl.when(role == r)
        def _():
            for run in items:
                run(add_up)

        waiting[r] += items

    wct[...] = jnp.zeros_like(wct)
    wct[0:4, :] = wcown[...]
    wc_copy.wait_recv()
    wct[16:20, :] = wcpar[...]

    @pl.loop(0, wct.shape[1] // 128)
    def _(i):
        part = pl.ds(pl.multiple_of(i * 128, 128), 128)
        wck[part, :] = wct[:, part].astype(f32).T.astype(bf16)

    compute(0, OWN, 2)
    collect(0, [own_items(half) for half in range(2)])

    hc_in.wait()
    for half in range(2):
        rows = jnp.dot(hcbuf[...], wbuf[half], preferred_element_type=f32)
        cbuf[:, 256 * half : 256 * (half + 1)] = rows[0:8] + rows[8:16]
    vbuf[t] = jnp.zeros_like(vbuf[t])

    def arrive(s):
        for d in dirs(s):
            h_copy(s, d).wait_recv()
        if OWN <= s + 2 < STEPS:
            for d in dirs(s + 2):
                h_copy(s + 2, d).start()

    lane = lax.broadcasted_iota(jnp.int32, (PIECE, 128), 1)

    def out_copies(q):
        rows = pl.ds(PIECE * q, PIECE)
        near = pltpu.make_async_copy(obuf.at[rows], out_hbm.at[rows], osem.at[q])
        far = remote(obuf.at[rows], out_hbm.at[rows], os_s.at[q], os_r.at[q], partner)
        return near, far

    def finish(q):
        for half in range(2):
            rows = pl.ds(0, ROWS[half])
            for side in range(2):
                remote(
                    pbuf.at[0, 0, rows],
                    zr.at[1 + side, half, q, rows],
                    zs.at[0, 0],
                    zrs.at[side, half, q],
                    (dp, t_other),
                ).wait_recv()
        marks = jnp.zeros((PIECE, 128), f32)
        for half in range(2):
            full = zr[0, half, q, 0:PIECE, :] + (zr[1, half, q, 0:PIECE, :] + zr[2, half, q, 0:PIECE, :])
            obuf[pl.ds(q * PIECE, PIECE), 256 * half : 256 * (half + 1)] = full.astype(bf16)
            vbuf[t, :, 256 * half : 256 * (half + 1)] += full.reshape(PIECE // 8, 8, 256).sum(0)
            for b in range(2):
                sums = full[:, 128 * b : 128 * (b + 1)].sum(-1, keepdims=True)
                marks = jnp.where(lane == 2 * half + b, sums, marks)
        near, far = out_copies(q)

        @pl.when(role == 0)
        def _():
            near.start()

        @pl.when(role == 1)
        def _():
            far.start()

        check = zr[0, 0, q, PIECE : PIECE + 8, 0:PIECE] + (
            zr[1, 0, q, PIECE : PIECE + 8, 0:PIECE] + zr[2, 0, q, PIECE : PIECE + 8, 0:PIECE]
        )
        rrbuf[q, :, 0:PIECE] = (check - marks.T[0:8]) * CHECK_BLOCK ** (-0.5)

    for low, high in ((0, 2), (2, 4), (4, 6), (6, 8), (8, 10), (10, 12), (12, 14), (14, 16), (16, 17), (17, 18), (18, 19)):
        for s in range(low, high):
            arrive(s)
        relay()
        n_j = 2 if low < 8 else 3 if low < 16 else 4
        compute(piece(low, 0), sum(len(dirs(s)) for s in range(low, high)), n_j)
        items = early_items if low < 8 else late_items
        collect(0, [items(low, high, half) for half in range(2)])
        if n_j > 2:
            collect(1, [items(low, high, half) for half in range(n_j - 2)])
        if high in (8, 16):
            half = high // 8 - 1
            w_copy[half].wait_recv()

            @pl.loop(0, (OWN + 3 * high) // 8)
            def _(i):
                mm(256 * i, 256, 8 * i, 2 + half)

            caught = [own_items(half), early_items(0, 8, half)]
            if half:
                caught.append(late_items(8, high, half))
            collect(1, caught)
        if high == STEPS - 1:

            @pl.loop(0, OWN)
            def _(i):
                finish(q_own + i)

            for few in ((0, 3), (4, 5)):

                @pl.loop(*few)
                def _(i):
                    finish(q_near + i)

    relay()
    for few in ((3, 4), (5, 8)):

        @pl.loop(*few)
        def _(i):
            finish(q_near + i)

    rr_far = remote(rrt, rrpar, fs.at[0], fr.at[0], partner)
    col_far = remote(vbuf.at[t], cpar, fs.at[1], fr.at[1], partner)

    @pl.when(role == 0)
    def _():
        vbuf[t] = cbuf[...] - vbuf[t]

    @pl.when(role == 1)
    def _():
        col_far.start()

    for q in range(2 * OWN):
        rrt[:, PIECE * q : PIECE * (q + 1)] = rrbuf[q, :, 0:PIECE]

    @pl.when(role == 1)
    def _():
        rr_far.start()
        col_far.wait()
        vbuf[t] = cbuf[...] - cpar[...]

    for d in range(1, 8):
        remote(vbuf.at[t], vbuf.at[t], vs.at[d - 1], vr.at[t], (dp, (t + d) % 8)).start()

    for s in range(STEPS):
        for d in dirs(s):
            h_copy(s, d).wait_send()
    wc_copy.wait_send()
    for j in range(2):
        w_copy[j].wait_send()

    @pl.loop(0, PIECES)
    def _(p):
        for half in range(2):
            core_copy(0, half, p).wait_send()

    def sent(half, p, zd, q):
        rows = pl.ds(0, ROWS[half])

        @pl.when(zd != z)
        def _():
            remote(
                pbuf.at[0, p, rows], zr.at[0, half, 0, rows], zs.at[half, p], zrs.at[0, half, 0], (dp, t_other)
            ).wait_send()

    for half in range(2):
        own_items(half)(sent)
        early_items(0, 8, half)(sent)
        late_items(8, STEPS, half)(sent)

    @pl.when(role == 0)
    def _():
        rr_ref[...] = rrt[0:4]

        @pl.loop(0, 2 * OWN)
        def _(q):
            out_copies(q)[0].wait()

    @pl.when(role == 1)
    def _():
        rr_far.wait()
        rr_ref[...] = rrpar[0:4]

        @pl.loop(0, 2 * OWN)
        def _(q):
            out_copies(q)[1].wait()

    for d in range(1, 8):
        src = (t + d) % 8
        remote(vbuf.at[src], vbuf.at[src], vs.at[d - 1], vr.at[src], (dp, src)).wait_recv()
    total = vbuf[0]
    for i in range(1, 8):
        total = total + vbuf[i]
    col_ref[...] = total.sum(0, keepdims=True) * 4096 ** (-0.5)
    for d in range(1, 8):
        remote(vbuf.at[t], vbuf.at[t], vs.at[d - 1], vr.at[t], (dp, (t + d) % 8)).wait_send()


def hand_over(out_in, rr_in, col_in, out_ref, rr_ref, col_ref):
    out_ref[...] = out_in[...]
    rr_ref[...] = rr_in[...]
    col_ref[...] = col_in[...]


def shards(hidden, hidden_check, down_weight, weight_check):
    f32, bf16 = jnp.float32, jnp.bfloat16
    k = hidden.shape[1]
    dma = pltpu.SemaphoreType.DMA
    shapes = (
        jax.ShapeDtypeStruct((512, 512), bf16),
        jax.ShapeDtypeStruct((4, 512), f32),
        jax.ShapeDtypeStruct((1, 512), f32),
    )
    vmem = pl.BlockSpec(memory_space=pltpu.VMEM)
    whole = pl.BlockSpec(memory_space=pl.ANY)
    results = pl.pallas_call(
        kernel,
        out_shape=shapes,
        in_specs=[whole] * 4,
        out_specs=(whole, vmem, vmem),
        scratch_shapes=[
            pltpu.VMEM((PIECE * PIECES, k), bf16),
            pltpu.VMEM((4, k, 256), bf16),
            pltpu.VMEM((16, k), bf16),
            pltpu.VMEM((4, k), bf16),
            pltpu.VMEM((4, k), bf16),
            pltpu.VMEM((128, k), bf16),
            pltpu.VMEM((k, 128), bf16),
            pltpu.VMEM((4, PIECES, 40, 256), f32),
            pltpu.VMEM((2, PIECES, 40, 256), f32),
            pltpu.VMEM((2, 16, 40, 256), f32),
            pltpu.VMEM((3, 2, 16, 40, 256), f32),
            pltpu.VMEM((512, 512), bf16),
            pltpu.VMEM((16, 8, 128), f32),
            pltpu.VMEM((8, 512), f32),
            pltpu.VMEM((8, 512), f32),
            pltpu.VMEM((8, 512), f32),
            pltpu.VMEM((8, 512), f32),
            pltpu.VMEM((8, 8, 512), f32),
            dma((5,)),
            dma((16,)),
            dma((STEPS, 3)),
            dma((STEPS, 3)),
            dma((3,)),
            dma((3,)),
            dma((2, PIECES)),
            dma((2, PIECES)),
            dma((2, PIECES)),
            dma((2, 2, 16)),
            dma((2, 16)),
            dma((16,)),
            dma((16,)),
            dma((2,)),
            dma((2,)),
            dma((7,)),
            dma((8,)),
        ],
        compiler_params=pltpu.CompilerParams(
            collective_id=0, has_side_effects=True, vmem_limit_bytes=60 * 1024 * 1024
        ),
    )(hidden, hidden_check, down_weight, weight_check.T)
    out, rr, col = pl.pallas_call(hand_over, out_shape=shapes, in_specs=[vmem] * 3, out_specs=(vmem,) * 3)(*results)
    return out, rr.T, col.reshape(512)


def solution(mesh):
    placed = (P("dp", "tensor"), P(None, "tensor"), P("tensor", "dp"), P("tensor", "dp"))
    return jax.shard_map(
        shards,
        mesh=mesh,
        in_specs=placed,
        out_specs=(P("tensor", "dp"), P("tensor", "dp"), P("dp")),
        check_vma=False,
    )
```

```python
import jax
import jax.numpy as jnp
from jax import lax
from jax.experimental import pallas as pl
from jax.experimental.pallas import tpu as pltpu
from jax.sharding import PartitionSpec as P

CHECK_BLOCK = 128
MESH = pl.DeviceIdType.MESH

PIECE = 32
OWN = 8
STEPS = 19
AHEAD = 4
BLOCK = 64
SLOTS = 34


def kernel(
    h_hbm, hc_hbm, w_hbm, wc_hbm,
    out_hbm, rr_ref, col_ref,
    hbuf, wbuf, hcbuf, wcown, wcpar, wct, wck, pbuf, rbuf, rl, zr, obuf, rrbuf, rrpart, rrt, rrpar, cbuf, colsum, nbuf, fbuf,
    lsem, osem, hs, hr, ws, wr, ds_s, ds_r, zs, zrs, rls, os_s, os_r, fs, fr, cs, cr, vs, vr,
):
    f32, bf16 = jnp.float32, jnp.bfloat16
    dp = lax.axis_index("dp")
    t = lax.axis_index("tensor")
    x, y = dp // 4, dp % 4
    z, c = t // 2, t % 2
    group = y // 2
    role = (c + group) % 2
    x_next = ((x + 1) % 4) * 4 + y
    x_prev = ((x + 3) % 4) * 4 + y
    y_near = x * 4 + (y // 2) * 2 + (y + 1) % 2
    y_far = x * 4 + 3 - y
    t_other = z * 2 + 1 - c
    partner = (y_far, t_other)

    def remote(src, dst, send, recv, dev):
        return pltpu.make_async_remote_copy(
            src_ref=src, dst_ref=dst, send_sem=send, recv_sem=recv, device_id=dev, device_id_type=MESH
        )

    h_in = pltpu.make_async_copy(h_hbm, hbuf.at[pl.ds(0, PIECE * OWN)], lsem.at[0])
    w_in = [pltpu.make_async_copy(w_hbm.at[:, pl.ds(256 * j, 256)], wbuf.at[j], lsem.at[1 + j]) for j in range(2)]
    hc_in = pltpu.make_async_copy(hc_hbm, hcbuf, lsem.at[3])
    wc_in = pltpu.make_async_copy(wc_hbm, wcown, lsem.at[4])
    h_in.start()
    wc_in.start()
    w_in[0].start()
    w_in[1].start()
    hc_in.start()

    barrier = pltpu.get_barrier_semaphore()
    peers = [(x_next, t), (x_prev, t), (y_near, t)]
    peers += [(dp, (t + d) % 8) for d in range(1, 8)]
    peers += [(y_far, (t + d) % 8) for d in range(8)]
    for peer in peers:
        pl.semaphore_signal(barrier, inc=1, device_id=peer, device_id_type=MESH)
    pl.semaphore_wait(barrier, len(peers))

    def row_of(s, d):
        if s is None:
            return PIECE * d
        if s == STEPS - 1:
            return PIECE * (OWN + 54 + d)
        return PIECE * (OWN + 6 * (s // 2) + 2 * d + s % 2)

    def source(s, d):
        if s < 8:
            return None, s
        if d == 2:
            if s < 10:
                return 0, s - 8
            k = (0, 1, 4, 5, 2, 3, 6, 7)[s - 10]
            return 8 + k % 4, k // 4
        if s < 12:
            return (s - 8, 0) if d == 0 else (s - 4, 1)
        return s - 11, 2

    def dirs(s):
        return range(3) if s < STEPS - 1 else range(2)

    def h_copy(s, d):
        dev = ((x_next, t), (x_prev, t), (y_near, t))[d]
        return remote(
            hbuf.at[pl.ds(row_of(*source(s, d)), PIECE)],
            hbuf.at[pl.ds(row_of(s, d), PIECE)],
            hs.at[s, d],
            hr.at[s, d],
            dev,
        )

    h_in.wait()
    for s in range(OWN):
        for d in dirs(s):
            h_copy(s, d).start()
    wc_in.wait()
    wc_copy = remote(wcown, wcpar, ws.at[2], wr.at[2], (y_far, t))
    wc_copy.start()
    w_copy = [remote(wbuf.at[j], wbuf.at[2 + j], ws.at[j], wr.at[j], (y_far, t)) for j in range(2)]
    for j in range(2):
        w_in[j].wait()
        w_copy[j].start()

    def core_copy(half, slot, rows, j=0):
        rows = pl.ds(0, rows)
        return remote(
            pbuf.at[j, slot, rows], rbuf.at[half, slot, rows], ds_s.at[half, slot], ds_r.at[half, slot], (dp, t_other)
        )

    def slot_of(pair, d):
        return 4 + 9 * d + pair

    def pair_slots(pair):
        if isinstance(pair, int) and pair == 4:
            return [(slot_of(4, 0), BLOCK), (slot_of(4, 1), BLOCK), (26, PIECE), (31, PIECE)]
        return [(slot_of(pair, d), BLOCK) for d in range(3)]

    own_slots = [(i, BLOCK) for i in range(4)]
    last_slots = [(32, PIECE), (33, PIECE)]

    def mm(row, slots, j):
        m = sum(n for _, n in slots)
        out = jnp.dot(hbuf[pl.ds(row, m), :], wbuf[j], preferred_element_type=f32)
        at = 0
        for slot, n in slots:
            pbuf[j, slot, 0:n, :] = out[at : at + n]
            at += n
        for half in range(2):

            @pl.when(j == 2 * (1 - role) + half)
            def _():
                for slot, n in slots:
                    core_copy(half, slot, n + 8, j).start()

    def checks(row, slots):
        m = sum(n for _, n in slots)
        out = jnp.dot(hbuf[pl.ds(row, m), :], wck[...], preferred_element_type=f32)
        at = 0
        for slot, n in slots:
            turned = out[at : at + n].T
            pbuf[0, slot, n : n + 8, 0:n] = turned[0:8]
            pbuf[2, slot, n : n + 8, 0:n] = turned[16:24]
            at += n

    def compute(row, slots, n_j):
        checks(row, slots)

        @pl.loop(0, n_j)
        def _(i):
            j = (i + 2 * (1 - role)) % 4 if n_j == 4 else i
            mm(row, slots, j)

    def parts(item):
        (h0, nh), (slot, ns), n, zd, q, way = item
        return (pl.ds(h0, nh), pl.ds(q, ns), pl.ds(0, n + 8)), (zd - z + 4) % 4

    def each(item):
        (h0, nh), (slot, ns), n, zd, q, way = item
        for half in range(h0, h0 + nh):
            for i in range(ns):
                yield half, slot + i, q + i, n + 8

    def send_to(r, item, dst, recv, to):
        (h0, nh), (slot, ns), n, zd, q, way = item
        src = pbuf.at[pl.ds(2 * r + h0, nh), pl.ds(slot, ns), pl.ds(0, n + 8)]
        return remote(src, dst, zs.at[h0, slot], recv, (dp, to * 2 + c))

    def to_relay(r, item):
        (h0, nh), (slot, ns), n, zd, q, way = item
        at, _ = parts(item)
        return send_to(r, item, rl.at[(way,) + at], rls.at[way, h0, q], (z + 1 + 2 * way) % 4)

    def to_owner(r, item, side):
        (h0, nh), (slot, ns), n, zd, q, way = item
        at, _ = parts(item)
        return send_to(r, item, zr.at[(1 + side,) + at], zrs.at[side, h0, q], zd)

    def add_up(r, item):
        for half, slot, q, rows in each(item):
            core_copy(half, slot, rows).wait_recv()
        way = item[-1]
        _, away = parts(item)

        @pl.when(away == 0)
        def _():
            for half, slot, q, rows in each(item):
                zr[0, half, q, 0:rows] = pbuf[2 * r + half, slot, 0:rows] + rbuf[half, slot, 0:rows]

        @pl.when(away != 0)
        def _():
            for half, slot, q, rows in each(item):
                pbuf[2 * r + half, slot, 0:rows] += rbuf[half, slot, 0:rows]

        @pl.when(away == 2)
        def _():
            to_relay(r, item).start()

        @pl.when(away == 3 - 2 * way)
        def _():
            to_owner(r, item, 1 - way).start()

    def pass_on(r, item):
        way = item[-1]
        _, away = parts(item)

        @pl.when(away == 1 + 2 * way)
        def _():
            to_relay(r, item).wait_recv()
            for half, slot, q, rows in each(item):
                pbuf[2 * r + half, slot, 0:rows] += rl[way, half, q, 0:rows]
            to_owner(r, item, way).start()

    def take(r, item):
        _, away = parts(item)

        @pl.when(away == 0)
        def _():
            for side in range(2):
                to_owner(r, item, side).wait_recv()

    def sent(r, item):
        _, away = parts(item)

        @pl.when(away != 0)
        def _():
            to_owner(r, item, 0).wait_send()

    def own_items(halves):
        def run(act):
            for i in (0, 2):
                act((halves, (i, 2), BLOCK, x, i, i // 2))

        return run

    def early_items(halves, low, n):
        def run(act):
            @pl.loop(0, 3)
            def _(d):
                for pair in range(low, low + 4 if n == 2 else low + 1, n):
                    zd = (x + 3 - 2 * d + d // 2) % 4
                    act((halves, (slot_of(pair, d), n), BLOCK, zd, pair + 4 * (d // 2), pair // 2))

        return run

    def late_items(halves, pair):
        def run(act):
            @pl.loop(0, 2)
            def _(d):
                if pair < 6:
                    act((halves, (slot_of(pair, d), 1), BLOCK, (x + 2) % 4, pair - 4 + 2 * d, pair % 2))
                else:
                    act((halves, (slot_of(pair, d), 1), BLOCK, (x + 3 - 2 * d + 4) % 4, pair - 1, pair % 2))

            if pair == 4:
                act((halves, (26, 1), PIECE, (x + 3) % 4, 4, 0))
                act((halves, (31, 1), PIECE, (x + 1) % 4, 4, 1))
            else:
                q = (4, 6, 5, 7)[pair - 5]
                act((halves, (slot_of(pair, 2), 1), BLOCK, (x + 2) % 4, q, (pair + 1) % 2))

        return run

    def last_items(halves):
        def run(act):
            @pl.loop(0, 2)
            def _(d):
                act((halves, (32 + d, 1), PIECE, (x + 3 - 2 * d) % 4, 8, 1))

        return run

    waiting = [[], []]
    gone = [[], []]

    def over(r, items, act):
        @pl.when(role == r)
        def _():
            for run in items:
                run(lambda item: act(r, item))

    def relay():
        for r in range(2):
            if waiting[r]:
                over(r, waiting[r], pass_on)
                gone[r] += waiting[r]
                waiting[r] = []

    def collect(r, items):
        over(r, items, add_up)
        waiting[r] += items

    wct[...] = jnp.zeros_like(wct)
    wct[0:4, :] = wcown[...]
    wc_copy.wait_recv()
    wct[16:20, :] = wcpar[...]

    @pl.loop(0, wct.shape[1] // 128)
    def _(i):
        part = pl.ds(pl.multiple_of(i * 128, 128), 128)
        wck[part, :] = wct[:, part].astype(f32).T.astype(bf16)

    both, first, second = (0, 2), (0, 1), (1, 1)
    compute(0, own_slots, 2)
    collect(0, [own_items(both)])

    hc_in.wait()
    for half in range(2):
        rows = jnp.dot(hcbuf[...], wbuf[half], preferred_element_type=f32)
        cbuf[t, :, 256 * half : 256 * (half + 1)] = rows[0:8] + rows[8:16]
    check_copies = [
        remote(cbuf.at[t], cbuf.at[t], cs.at[d - 1], cr.at[t], (dp, (t + d) % 8)) for d in range(1, 8)
    ]
    for copy in check_copies:
        copy.start()
    colsum[...] = jnp.zeros_like(colsum)

    def arrive(s):
        for d in dirs(s):
            h_copy(s, d).wait_recv()
        for later in range(OWN, STEPS):
            for d in dirs(later):
                if max(later - AHEAD, source(later, d)[0]) == s:
                    h_copy(later, d).start()

    def out_copies(q, row, n):
        rows = pl.ds(pl.multiple_of(row, PIECE), n)
        near = pltpu.make_async_copy(obuf.at[rows], out_hbm.at[rows], osem.at[q])
        far = remote(obuf.at[rows], out_hbm.at[rows], os_s.at[q], os_r.at[q], partner)
        return near, far

    def finish(q, row, n):
        lane = lax.broadcasted_iota(jnp.int32, (n, 128), 1)
        marks = jnp.zeros((n, 128), f32)
        for half in range(2):
            full = zr[0, half, q, 0:n, :] + (zr[1, half, q, 0:n, :] + zr[2, half, q, 0:n, :])
            obuf[pl.ds(pl.multiple_of(row, PIECE), n), 256 * half : 256 * (half + 1)] = full.astype(bf16)
            colsum[:, 256 * half : 256 * (half + 1)] += full.reshape(n // 8, 8, 256).sum(0)
            for b in range(2):
                sums = full[:, 128 * b : 128 * (b + 1)].sum(-1, keepdims=True)
                marks = jnp.where(lane == 2 * half + b, sums, marks)
        near, far = out_copies(q, row, n)

        @pl.when(role == 0)
        def _():
            near.start()

        @pl.when(role == 1)
        def _():
            far.start()

        check = zr[0, 0, q, n : n + 8, 0:n] + (zr[1, 0, q, n : n + 8, 0:n] + zr[2, 0, q, n : n + 8, 0:n])
        rrbuf[q, :, 0:n] = (check - marks.T[0:8]) * CHECK_BLOCK ** (-0.5)

    row_own = (y % 2) * 256
    row_near = ((y + 1) % 2) * 256
    apart = (z - x + 4) % 2

    def finish_near(act, late):
        @pl.when(apart == 0)
        def _():
            @pl.loop(7 if late else 4, 8 if late else 7)
            def _(q):
                act(q, row_near + BLOCK * (q - 4), BLOCK)

        @pl.when(apart == 1)
        def _():
            act(8 if late else 4, row_near + (224 if late else 0), PIECE)

            @pl.loop(7 if late else 5, 8 if late else 7)
            def _(q):
                act(q, row_near + PIECE + BLOCK * (q - 5), BLOCK)

    def finish_own(act):
        @pl.loop(0, 4)
        def _(q):
            act(q, row_own + BLOCK * q, BLOCK)

    def catch_up(pairs, half):
        w_copy[half].wait_recv()
        mm(0, own_slots, 2 + half)
        for low, high in pairs:
            if high - low == 1:
                mm(row_of(2 * low, 0), pair_slots(low), 2 + half)
            else:

                @pl.loop(low, high)
                def _(pair):
                    mm(PIECE * OWN + 192 * pair, pair_slots(pair), 2 + half)

    for pair in range(9):
        arrive(2 * pair)
        arrive(2 * pair + 1)
        relay()
        compute(row_of(2 * pair, 0), pair_slots(pair), 2 if pair < 4 else 3 if pair < 8 else 4)
        if pair < 4:
            if pair == 3:
                catch_up([(0, 4)], 0)
            collect(0, [early_items(both, pair, 1)])
            if pair == 3:
                collect(1, [own_items(first), early_items(first, 0, 2)])
        else:
            if pair == 7:
                catch_up([(0, 4), (4, 5), (5, 8)], 1)
            collect(0, [late_items(both, pair)])
            collect(1, [late_items(first if pair < 8 else both, pair)])
            if pair == 7:
                collect(1, [own_items(second), early_items(second, 0, 2)] + [late_items(second, k) for k in range(4, 8)])
                relay()

    early_gone = [list(items) for items in gone]
    for r in range(2):
        over(r, early_gone[r], take)
    finish_own(finish)
    finish_near(finish, False)
    relay()
    arrive(18)
    compute(row_of(18, 0), last_slots, 4)
    for r in range(2):
        collect(r, [last_items(both)])
    relay()
    for r in range(2):
        over(r, gone[r][len(early_gone[r]) :], take)
    finish_near(finish, True)

    near_copies = [remote(colsum, nbuf.at[z], vs.at[d], vr.at[z], (dp, (t + d) % 8)) for d in range(1, 8)]
    far_copies = [remote(colsum, fbuf.at[z], vs.at[d], vr.at[4 + z], (y_far, (t + d) % 8)) for d in range(8)]
    rr_far = remote(rrt, rrpar, fs.at[0], fr.at[0], partner)

    @pl.when(role == 0)
    def _():
        for copy in near_copies:
            copy.start()
        nbuf[z] = colsum[...]

    @pl.when(role == 1)
    def _():
        for copy in far_copies:
            copy.start()

    for q in range(4):
        rrpart[0, :, BLOCK * q : BLOCK * (q + 1)] = rrbuf[q, :, 0:BLOCK]

    @pl.when(apart == 0)
    def _():
        for q in range(4):
            rrpart[1, :, BLOCK * q : BLOCK * (q + 1)] = rrbuf[4 + q, :, 0:BLOCK]

    @pl.when(apart == 1)
    def _():
        rrpart[1, :, 0:PIECE] = rrbuf[4, :, 0:PIECE]
        for q in range(3):
            rrpart[1, :, PIECE + BLOCK * q : PIECE + BLOCK * (q + 1)] = rrbuf[5 + q, :, 0:BLOCK]
        rrpart[1, :, 256 - PIECE : 256] = rrbuf[8, :, 0:PIECE]

    rrt[:, pl.ds(pl.multiple_of(row_own, 256), 256)] = rrpart[0]
    rrt[:, pl.ds(pl.multiple_of(row_near, 256), 256)] = rrpart[1]

    @pl.when(role == 0)
    def _():
        rr_ref[...] = rrt[0:4]

    @pl.when(role == 1)
    def _():
        rr_far.start()

    for s in range(STEPS):
        for d in dirs(s):
            h_copy(s, d).wait_send()
    wc_copy.wait_send()
    for j in range(2):
        w_copy[j].wait_send()
    for copy in check_copies:
        copy.wait_send()
    def given(slot, n):
        for half in range(2):
            core_copy(half, slot, n + 8).wait_send()

    @pl.loop(0, 26)
    def _(slot):
        given(slot, BLOCK)

    @pl.loop(27, 31)
    def _(slot):
        given(slot, BLOCK)

    for slot in (26, 31, 32, 33):
        given(slot, PIECE)
    for r in range(2):
        over(r, gone[r], sent)

    def written(side):
        def act(q, row, n):
            out_copies(q, row, n)[side].wait()

        finish_own(act)
        for late in (False, True):
            finish_near(act, late)

    total = cbuf[t]
    for d in range(1, 8):
        src = (t + d) % 8
        remote(cbuf.at[src], cbuf.at[src], cs.at[d - 1], cr.at[src], (dp, src)).wait_recv()
        total = total + cbuf[src]

    @pl.when(role == 0)
    def _():
        for d in range(1, 4):
            src = (z + d) % 4
            remote(colsum, nbuf.at[src], vs.at[0], vr.at[src], (dp, t_other)).wait_recv()

    @pl.when(role == 1)
    def _():
        for src in range(4):
            remote(colsum, nbuf.at[src], vs.at[0], vr.at[src], (dp, t_other)).wait_recv()

    for src in range(4):
        remote(colsum, fbuf.at[src], vs.at[0], vr.at[4 + src], partner).wait_recv()
    sums = (nbuf[0] + nbuf[1]) + (nbuf[2] + nbuf[3])
    sums = sums + ((fbuf[0] + fbuf[1]) + (fbuf[2] + fbuf[3]))
    col_ref[...] = (total - sums).sum(0, keepdims=True) * 4096 ** (-0.5)

    @pl.when(role == 0)
    def _():
        written(0)

        for copy in near_copies:
            copy.wait_send()

    @pl.when(role == 1)
    def _():
        rr_far.wait()
        rr_ref[...] = rrpar[0:4]

        written(1)

        for copy in far_copies:
            copy.wait_send()


def hand_over(out_in, rr_in, col_in, out_ref, rr_ref, col_ref):
    out_ref[...] = out_in[...]
    rr_ref[...] = rr_in[...]
    col_ref[...] = col_in[...]


def shards(hidden, hidden_check, down_weight, weight_check):
    f32, bf16 = jnp.float32, jnp.bfloat16
    k = hidden.shape[1]
    dma = pltpu.SemaphoreType.DMA
    shapes = (
        jax.ShapeDtypeStruct((512, 512), bf16),
        jax.ShapeDtypeStruct((4, 512), f32),
        jax.ShapeDtypeStruct((1, 512), f32),
    )
    vmem = pl.BlockSpec(memory_space=pltpu.VMEM)
    whole = pl.BlockSpec(memory_space=pl.ANY)
    results = pl.pallas_call(
        kernel,
        out_shape=shapes,
        in_specs=[whole] * 4,
        out_specs=(whole, vmem, vmem),
        scratch_shapes=[
            pltpu.VMEM((2048, k), bf16),
            pltpu.VMEM((4, k, 256), bf16),
            pltpu.VMEM((16, k), bf16),
            pltpu.VMEM((4, k), bf16),
            pltpu.VMEM((4, k), bf16),
            pltpu.VMEM((128, k), bf16),
            pltpu.VMEM((k, 128), bf16),
            pltpu.VMEM((4, SLOTS, BLOCK + 8, 256), f32),
            pltpu.VMEM((2, SLOTS, BLOCK + 8, 256), f32),
            pltpu.VMEM((2, 2, 9, BLOCK + 8, 256), f32),
            pltpu.VMEM((3, 2, 9, BLOCK + 8, 256), f32),
            pltpu.VMEM((512, 512), bf16),
            pltpu.VMEM((9, 8, 128), f32),
            pltpu.VMEM((2, 8, 256), f32),
            pltpu.VMEM((8, 512), f32),
            pltpu.VMEM((8, 512), f32),
            pltpu.VMEM((8, 8, 512), f32),
            pltpu.VMEM((8, 512), f32),
            pltpu.VMEM((4, 8, 512), f32),
            pltpu.VMEM((4, 8, 512), f32),
            dma((5,)),
            dma((9,)),
            dma((STEPS, 3)),
            dma((STEPS, 3)),
            dma((3,)),
            dma((3,)),
            dma((2, SLOTS)),
            dma((2, SLOTS)),
            dma((2, SLOTS)),
            dma((2, 2, 9)),
            dma((2, 2, 9)),
            dma((9,)),
            dma((9,)),
            dma((1,)),
            dma((1,)),
            dma((7,)),
            dma((8,)),
            dma((8,)),
            dma((8,)),
        ],
        compiler_params=pltpu.CompilerParams(
            collective_id=0, has_side_effects=True, vmem_limit_bytes=60 * 1024 * 1024
        ),
    )(hidden, hidden_check, down_weight, weight_check.T)
    out, rr, col = pl.pallas_call(hand_over, out_shape=shapes, in_specs=[vmem] * 3, out_specs=(vmem,) * 3)(*results)
    return out, rr.T, col.reshape(512)


def solution(mesh):
    placed = (P("dp", "tensor"), P(None, "tensor"), P("tensor", "dp"), P("tensor", "dp"))
    return jax.shard_map(
        shards,
        mesh=mesh,
        in_specs=placed,
        out_specs=(P("tensor", "dp"), P("tensor", "dp"), P("dp")),
        check_vma=False,
    )
```

```python
import jax
import jax.numpy as jnp
from jax import lax
from jax.experimental import pallas as pl
from jax.experimental.pallas import tpu as pltpu
from jax.sharding import PartitionSpec as P

CHECK_BLOCK = 128
MESH = pl.DeviceIdType.MESH

PIECE = 32
OWN = 8
STEPS = 19
AHEAD = 4
BLOCK = 64
SLOTS = 34


def kernel(
    h_hbm, hc_hbm, w_hbm, wc_hbm,
    out_hbm, rr_ref, col_ref,
    hbuf, wbuf, hcbuf, wcown, wcpar, wct, wck, pbuf, rbuf, zr, obuf, rrbuf, rrpart, rrt, rrpar, cbuf, colsum, nbuf, fbuf,
    lsem, osem, hs, hr, ws, wr, ds_s, ds_r, zs, zrs, os_s, os_r, fs, fr, cs, cr, vs, vr,
):
    f32, bf16 = jnp.float32, jnp.bfloat16
    dp = lax.axis_index("dp")
    t = lax.axis_index("tensor")
    x, y = dp // 4, dp % 4
    z, c = t // 2, t % 2
    group = y // 2
    role = (c + group) % 2
    x_next = ((x + 1) % 4) * 4 + y
    x_prev = ((x + 3) % 4) * 4 + y
    y_near = x * 4 + (y // 2) * 2 + (y + 1) % 2
    y_far = x * 4 + 3 - y
    t_other = z * 2 + 1 - c
    partner = (y_far, t_other)

    def remote(src, dst, send, recv, dev):
        return pltpu.make_async_remote_copy(
            src_ref=src, dst_ref=dst, send_sem=send, recv_sem=recv, device_id=dev, device_id_type=MESH
        )

    h_in = pltpu.make_async_copy(h_hbm, hbuf.at[pl.ds(0, PIECE * OWN)], lsem.at[0])
    w_in = [pltpu.make_async_copy(w_hbm.at[:, pl.ds(256 * j, 256)], wbuf.at[j], lsem.at[1 + j]) for j in range(2)]
    hc_in = pltpu.make_async_copy(hc_hbm, hcbuf, lsem.at[3])
    wc_in = pltpu.make_async_copy(wc_hbm, wcown, lsem.at[4])
    h_in.start()
    wc_in.start()
    w_in[0].start()
    w_in[1].start()
    hc_in.start()

    barrier = pltpu.get_barrier_semaphore()
    peers = [(x_next, t), (x_prev, t), (y_near, t)]
    peers += [(dp, (t + d) % 8) for d in range(1, 8)]
    peers += [(y_far, (t + d) % 8) for d in range(8)]
    for peer in peers:
        pl.semaphore_signal(barrier, inc=1, device_id=peer, device_id_type=MESH)
    pl.semaphore_wait(barrier, len(peers))

    def row_of(s, d):
        if s is None:
            return PIECE * d
        if s == STEPS - 1:
            return PIECE * (OWN + 54 + d)
        return PIECE * (OWN + 6 * (s // 2) + 2 * d + s % 2)

    def source(s, d):
        if s < 8:
            return None, s
        if d == 2:
            if s < 10:
                return 0, s - 8
            k = (0, 1, 4, 5, 2, 3, 6, 7)[s - 10]
            return 8 + k % 4, k // 4
        if s < 12:
            return (s - 8, 0) if d == 0 else (s - 4, 1)
        return s - 11, 2

    def dirs(s):
        return range(3) if s < STEPS - 1 else range(2)

    def h_copy(s, d):
        dev = ((x_next, t), (x_prev, t), (y_near, t))[d]
        return remote(
            hbuf.at[pl.ds(row_of(*source(s, d)), PIECE)],
            hbuf.at[pl.ds(row_of(s, d), PIECE)],
            hs.at[s, d],
            hr.at[s, d],
            dev,
        )

    h_in.wait()
    for s in range(OWN):
        for d in dirs(s):
            h_copy(s, d).start()
    wc_in.wait()
    wc_copy = remote(wcown, wcpar, ws.at[2], wr.at[2], (y_far, t))
    wc_copy.start()
    lows, highs = pl.ds(0, 128), pl.ds(128, 128)
    w_copy = [
        remote(wbuf.at[0], wbuf.at[2], ws.at[0], wr.at[0], (y_far, t)),
        remote(wbuf.at[1, :, lows], wbuf.at[3, :, lows], ws.at[1], wr.at[1], (y_far, t)),
        remote(wbuf.at[1, :, highs], wbuf.at[3, :, highs], ws.at[3], wr.at[3], (y_far, t)),
    ]
    for copy in w_in:
        copy.wait()
    for copy in w_copy:
        copy.start()

    both, first = (0, 2, 0, 256, 0), (0, 1, 0, 256, 0)
    third, fourth = (1, 1, 0, 128, 1), (1, 1, 128, 128, 2)

    def core_copy(half, slot, rows, j=0, lane=0, lanes=256):
        tag = half + lane // 128
        at = (slot, pl.ds(0, rows), pl.ds(lane, lanes))
        return remote(
            pbuf.at[(j,) + at], rbuf.at[(half,) + at], ds_s.at[tag, slot], ds_r.at[tag, slot], (dp, t_other)
        )

    def slot_of(pair, d):
        return 4 + 9 * d + pair

    def pair_slots(pair):
        if isinstance(pair, int) and pair == 4:
            return [(slot_of(4, 0), BLOCK), (slot_of(4, 1), BLOCK), (26, PIECE), (31, PIECE)]
        return [(slot_of(pair, d), BLOCK) for d in range(3)]

    own_slots = [(i, BLOCK) for i in range(4)]
    last_slots = [(32, PIECE), (33, PIECE)]

    def mm_part(row, slots, part):
        half, _, lane, lanes, _ = part
        m = sum(n for _, n in slots)
        out = jnp.dot(hbuf[pl.ds(row, m), :], wbuf[3, :, lane : lane + lanes], preferred_element_type=f32)
        at = 0
        for slot, n in slots:
            pbuf[3, slot, 0:n, lane : lane + lanes] = out[at : at + n]
            at += n

        @pl.when(role == 0)
        def _():
            for slot, n in slots:
                core_copy(1, slot, n, 3, lane, lanes).start()

    def mm(row, slots, j):
        m = sum(n for _, n in slots)
        out = jnp.dot(hbuf[pl.ds(row, m), :], wbuf[j], preferred_element_type=f32)
        at = 0
        for slot, n in slots:
            pbuf[j, slot, 0:n, :] = out[at : at + n]
            at += n
        for half in range(2):

            @pl.when(j == 2 * (1 - role) + half)
            def _():
                for slot, n in slots:
                    core_copy(half, slot, n + 8, j).start()

    def checks(row, slots):
        m = sum(n for _, n in slots)
        out = jnp.dot(hbuf[pl.ds(row, m), :], wck[...], preferred_element_type=f32)
        at = 0
        for slot, n in slots:
            turned = out[at : at + n].T
            pbuf[0, slot, n : n + 8, 0:n] = turned[0:8]
            pbuf[2, slot, n : n + 8, 0:n] = turned[16:24]
            at += n

    def compute(row, slots, n_j):
        checks(row, slots)

        @pl.loop(0, n_j)
        def _(i):
            j = (i + 2 * (1 - role)) % 4 if n_j == 4 else i
            mm(row, slots, j)

    def rows_of(item):
        return item[2] + (8 if item[0][0] == 0 else 0)

    def away(item):
        return (item[3] - z + 4) % 4

    def each(item):
        (h0, nh, lane, lanes, tag), (slot, ns), n, zd, q = item
        cols = slice(lane, lane + lanes)
        for half in range(h0, h0 + nh):
            for i in range(ns):
                yield half, slot + i, q + i, rows_of(item), cols

    def to_owner(r, item, side):
        (h0, nh, lane, lanes, tag), (slot, ns), n, zd, q = item
        tail = (pl.ds(0, rows_of(item)), pl.ds(lane, lanes))
        src = pbuf.at[(pl.ds(2 * r + h0, nh), pl.ds(slot, ns)) + tail]
        dst = zr.at[(1 + side, pl.ds(h0, nh), pl.ds(q, ns)) + tail]
        return remote(src, dst, zs.at[tag, slot], zrs.at[side, tag, q], (dp, zd * 2 + c))

    def add_up(r, item):
        lane, lanes = item[0][2:4]
        for half, slot, q, rows, cols in each(item):
            core_copy(half, slot, rows if lanes == 128 else item[2] + 8, 0, lane, lanes).wait_recv()

        @pl.when(away(item) == 0)
        def _():
            for half, slot, q, rows, cols in each(item):
                zr[0, half, q, 0:rows, cols] = pbuf[2 * r + half, slot, 0:rows, cols] + rbuf[half, slot, 0:rows, cols]

        @pl.when(away(item) != 0)
        def _():
            for half, slot, q, rows, cols in each(item):
                pbuf[2 * r + half, slot, 0:rows, cols] += rbuf[half, slot, 0:rows, cols]
            to_owner(r, item, away(item) - 1).start()

    def take(r, item):
        @pl.when(away(item) == 0)
        def _():
            for side in range(3):
                to_owner(r, item, side).wait_recv()

    def sent(r, item):
        @pl.when(away(item) != 0)
        def _():
            to_owner(r, item, 0).wait_send()

    def own_items(halves):
        def run(act):
            for i in (0, 2):
                act((halves, (i, 2), BLOCK, x, i))

        return run

    def early_items(halves, low, n):
        def run(act):
            @pl.loop(0, 3)
            def _(d):
                for pair in range(low, low + 4 if n == 2 else low + 1, n):
                    zd = (x + 3 - 2 * d + d // 2) % 4
                    act((halves, (slot_of(pair, d), n), BLOCK, zd, pair + 4 * (d // 2)))

        return run

    def late_items(halves, pair):
        def run(act):
            @pl.loop(0, 2)
            def _(d):
                if pair < 6:
                    act((halves, (slot_of(pair, d), 1), BLOCK, (x + 2) % 4, pair - 4 + 2 * d))
                else:
                    act((halves, (slot_of(pair, d), 1), BLOCK, (x + 3 - 2 * d + 4) % 4, pair - 1))

            if pair == 4:
                act((halves, (26, 1), PIECE, (x + 3) % 4, 4))
                act((halves, (31, 1), PIECE, (x + 1) % 4, 4))
            else:
                q = (4, 6, 5, 7)[pair - 5]
                act((halves, (slot_of(pair, 2), 1), BLOCK, (x + 2) % 4, q))

        return run

    def last_items(halves):
        def run(act):
            @pl.loop(0, 2)
            def _(d):
                act((halves, (32 + d, 1), PIECE, (x + 3 - 2 * d) % 4, 8))

        return run

    gone = [[], []]

    def over(r, items, act):
        @pl.when(role == r)
        def _():
            for run in items:
                run(lambda item: act(r, item))

    def collect(r, items, pair=0):
        over(r, items, add_up)
        gone[r] += [(run, pair) for run in items]

    wct[...] = jnp.zeros_like(wct)
    wct[0:4, :] = wcown[...]
    wc_copy.wait_recv()
    wct[16:20, :] = wcpar[...]

    @pl.loop(0, wct.shape[1] // 128)
    def _(i):
        part = pl.ds(pl.multiple_of(i * 128, 128), 128)
        wck[part, :] = wct[:, part].astype(f32).T.astype(bf16)

    compute(0, own_slots, 2)
    collect(0, [own_items(both)])

    hc_in.wait()
    for half in range(2):
        rows = jnp.dot(hcbuf[...], wbuf[half], preferred_element_type=f32)
        cbuf[t, :, 256 * half : 256 * (half + 1)] = rows[0:8] + rows[8:16]
    check_copies = [
        remote(cbuf.at[t], cbuf.at[t], cs.at[d - 1], cr.at[t], (dp, (t + d) % 8)) for d in range(1, 8)
    ]
    for copy in check_copies:
        copy.start()
    colsum[...] = jnp.zeros_like(colsum)

    def arrive(s):
        for d in dirs(s):
            h_copy(s, d).wait_recv()
        for later in range(OWN, STEPS):
            for d in dirs(later):
                if max(later - AHEAD, source(later, d)[0]) == s:
                    h_copy(later, d).start()

    def out_copies(q, row, n):
        rows = pl.ds(pl.multiple_of(row, PIECE), n)
        near = pltpu.make_async_copy(obuf.at[rows], out_hbm.at[rows], osem.at[q])
        far = remote(obuf.at[rows], out_hbm.at[rows], os_s.at[q], os_r.at[q], partner)
        return near, far

    def finish(q, row, n):
        lane = lax.broadcasted_iota(jnp.int32, (n, 128), 1)
        marks = jnp.zeros((n, 128), f32)
        for half in range(2):
            full = (zr[0, half, q, 0:n, :] + zr[1, half, q, 0:n, :]) + (zr[2, half, q, 0:n, :] + zr[3, half, q, 0:n, :])
            obuf[pl.ds(pl.multiple_of(row, PIECE), n), 256 * half : 256 * (half + 1)] = full.astype(bf16)
            colsum[:, 256 * half : 256 * (half + 1)] += full.reshape(n // 8, 8, 256).sum(0)
            for b in range(2):
                sums = full[:, 128 * b : 128 * (b + 1)].sum(-1, keepdims=True)
                marks = jnp.where(lane == 2 * half + b, sums, marks)
        near, far = out_copies(q, row, n)

        @pl.when(role == 0)
        def _():
            near.start()

        @pl.when(role == 1)
        def _():
            far.start()

        check = (zr[0, 0, q, n : n + 8, 0:n] + zr[1, 0, q, n : n + 8, 0:n]) + (
            zr[2, 0, q, n : n + 8, 0:n] + zr[3, 0, q, n : n + 8, 0:n]
        )
        rrbuf[q, :, 0:n] = (check - marks.T[0:8]) * CHECK_BLOCK ** (-0.5)

    row_own = (y % 2) * 256
    row_near = ((y + 1) % 2) * 256
    apart = (z - x + 4) % 2

    def finish_near(act, late):
        @pl.when(apart == 0)
        def _():
            @pl.loop(7 if late else 4, 8 if late else 7)
            def _(q):
                act(q, row_near + BLOCK * (q - 4), BLOCK)

        @pl.when(apart == 1)
        def _():
            act(8 if late else 4, row_near + (224 if late else 0), PIECE)

            @pl.loop(7 if late else 5, 8 if late else 7)
            def _(q):
                act(q, row_near + PIECE + BLOCK * (q - 5), BLOCK)

    def finish_own(act):
        @pl.loop(0, 4)
        def _(q):
            act(q, row_own + BLOCK * q, BLOCK)

    def early_mm(one):
        one(0, own_slots)

        @pl.loop(0, 4)
        def _(pair):
            one(PIECE * OWN + 192 * pair, pair_slots(pair))

    def late_mm(one, low, high):
        for pair in range(low, min(high, 5)):
            one(row_of(2 * pair, 0), pair_slots(pair))
        if high > 5:

            @pl.loop(max(low, 5), high)
            def _(pair):
                one(PIECE * OWN + 192 * pair, pair_slots(pair))

    for pair in range(9):
        arrive(2 * pair)
        arrive(2 * pair + 1)
        row, slots = row_of(2 * pair, 0), pair_slots(pair)
        compute(row, slots, 2 if pair < 4 else 3 if pair < 8 else 4)
        if pair < 4:
            collect(0, [early_items(both, pair, 1)])
        else:
            collect(0, [late_items(both, pair)], pair)
            collect(1, [late_items(first if pair < 8 else both, pair)], pair)
        if pair == 3:
            w_copy[0].wait_recv()
            early_mm(lambda row, slots: mm(row, slots, 2))
            collect(1, [own_items(first), early_items(first, 0, 2)])
        for at, part in ((5, third), (7, fourth)):
            if pair == at:
                w_copy[part[-1]].wait_recv()
                early_mm(lambda row, slots: mm_part(row, slots, part))
                collect(1, [own_items(part), early_items(part, 0, 2)])
                late_mm(lambda row, slots: mm_part(row, slots, part), 4, pair + 1)
                collect(1, [late_items(part, k) for k in range(4, pair + 1)])
            elif at < pair < 8 and part == third:
                mm_part(row, slots, part)
                collect(1, [late_items(part, pair)])
    early_gone = [[run for run, pair in gone[r] if pair < 8] for r in range(2)]
    late_gone = [[run for run, pair in gone[r] if pair == 8] for r in range(2)]

    arrive(18)
    compute(row_of(18, 0), last_slots, 4)
    for r in range(2):
        collect(r, [last_items(both)], 8)
        late_gone[r].append(last_items(both))
    for r in range(2):
        over(r, early_gone[r], take)
    finish_own(finish)
    finish_near(finish, False)
    for r in range(2):
        over(r, late_gone[r], take)
    finish_near(finish, True)

    near_copies = [remote(colsum, nbuf.at[z], vs.at[d], vr.at[z], (dp, (t + d) % 8)) for d in range(1, 8)]
    far_copies = [remote(colsum, fbuf.at[z], vs.at[d], vr.at[4 + z], (y_far, (t + d) % 8)) for d in range(8)]
    rr_far = remote(rrt, rrpar, fs.at[0], fr.at[0], partner)

    @pl.when(role == 0)
    def _():
        for copy in near_copies:
            copy.start()
        nbuf[z] = colsum[...]

    @pl.when(role == 1)
    def _():
        for copy in far_copies:
            copy.start()

    for q in range(4):
        rrpart[0, :, BLOCK * q : BLOCK * (q + 1)] = rrbuf[q, :, 0:BLOCK]

    @pl.when(apart == 0)
    def _():
        for q in range(4):
            rrpart[1, :, BLOCK * q : BLOCK * (q + 1)] = rrbuf[4 + q, :, 0:BLOCK]

    @pl.when(apart == 1)
    def _():
        rrpart[1, :, 0:PIECE] = rrbuf[4, :, 0:PIECE]
        for q in range(3):
            rrpart[1, :, PIECE + BLOCK * q : PIECE + BLOCK * (q + 1)] = rrbuf[5 + q, :, 0:BLOCK]
        rrpart[1, :, 256 - PIECE : 256] = rrbuf[8, :, 0:PIECE]

    rrt[:, pl.ds(pl.multiple_of(row_own, 256), 256)] = rrpart[0]
    rrt[:, pl.ds(pl.multiple_of(row_near, 256), 256)] = rrpart[1]

    @pl.when(role == 0)
    def _():
        rr_ref[...] = rrt[0:4]

    @pl.when(role == 1)
    def _():
        rr_far.start()

    for s in range(STEPS):
        for d in dirs(s):
            h_copy(s, d).wait_send()
    wc_copy.wait_send()
    for copy in w_copy:
        copy.wait_send()
    for copy in check_copies:
        copy.wait_send()
    def given(slot, n, split=True):
        core_copy(0, slot, n + 8).wait_send()
        if not split:
            core_copy(1, slot, n + 8).wait_send()
            return

        @pl.when(role == 1)
        def _():
            core_copy(1, slot, n + 8).wait_send()

        @pl.when(role == 0)
        def _():
            for part in (third, fourth):
                core_copy(1, slot, n, 3, part[2], part[3]).wait_send()

    for low, high in ((0, 12), (13, 21), (22, 26), (27, 30)):

        @pl.loop(low, high)
        def _(slot):
            given(slot, BLOCK)

    for slot in (12, 21, 30):
        given(slot, BLOCK, False)
    for slot in (26, 31):
        given(slot, PIECE)
    for slot in (32, 33):
        given(slot, PIECE, False)
    for r in range(2):
        over(r, early_gone[r] + late_gone[r], sent)

    def written(side):
        def act(q, row, n):
            out_copies(q, row, n)[side].wait()

        finish_own(act)
        for late in (False, True):
            finish_near(act, late)

    total = cbuf[t]
    for d in range(1, 8):
        src = (t + d) % 8
        remote(cbuf.at[src], cbuf.at[src], cs.at[d - 1], cr.at[src], (dp, src)).wait_recv()
        total = total + cbuf[src]

    @pl.when(role == 0)
    def _():
        for d in range(1, 4):
            src = (z + d) % 4
            remote(colsum, nbuf.at[src], vs.at[0], vr.at[src], (dp, t_other)).wait_recv()

    @pl.when(role == 1)
    def _():
        for src in range(4):
            remote(colsum, nbuf.at[src], vs.at[0], vr.at[src], (dp, t_other)).wait_recv()

    for src in range(4):
        remote(colsum, fbuf.at[src], vs.at[0], vr.at[4 + src], partner).wait_recv()
    sums = (nbuf[0] + nbuf[1]) + (nbuf[2] + nbuf[3])
    sums = sums + ((fbuf[0] + fbuf[1]) + (fbuf[2] + fbuf[3]))
    col_ref[...] = (total - sums).sum(0, keepdims=True) * 4096 ** (-0.5)

    @pl.when(role == 0)
    def _():
        written(0)

        for copy in near_copies:
            copy.wait_send()

    @pl.when(role == 1)
    def _():
        rr_far.wait()
        rr_ref[...] = rrpar[0:4]

        written(1)

        for copy in far_copies:
            copy.wait_send()


def hand_over(out_in, rr_in, col_in, out_ref, rr_ref, col_ref):
    out_ref[...] = out_in[...]
    rr_ref[...] = rr_in[...]
    col_ref[...] = col_in[...]


def shards(hidden, hidden_check, down_weight, weight_check):
    f32, bf16 = jnp.float32, jnp.bfloat16
    k = hidden.shape[1]
    dma = pltpu.SemaphoreType.DMA
    shapes = (
        jax.ShapeDtypeStruct((512, 512), bf16),
        jax.ShapeDtypeStruct((4, 512), f32),
        jax.ShapeDtypeStruct((1, 512), f32),
    )
    vmem = pl.BlockSpec(memory_space=pltpu.VMEM)
    whole = pl.BlockSpec(memory_space=pl.ANY)
    results = pl.pallas_call(
        kernel,
        out_shape=shapes,
        in_specs=[whole] * 4,
        out_specs=(whole, vmem, vmem),
        scratch_shapes=[
            pltpu.VMEM((2048, k), bf16),
            pltpu.VMEM((4, k, 256), bf16),
            pltpu.VMEM((16, k), bf16),
            pltpu.VMEM((4, k), bf16),
            pltpu.VMEM((4, k), bf16),
            pltpu.VMEM((128, k), bf16),
            pltpu.VMEM((k, 128), bf16),
            pltpu.VMEM((4, SLOTS, BLOCK + 8, 256), f32),
            pltpu.VMEM((2, SLOTS, BLOCK + 8, 256), f32),
            pltpu.VMEM((4, 2, 9, BLOCK + 8, 256), f32),
            pltpu.VMEM((512, 512), bf16),
            pltpu.VMEM((9, 8, 128), f32),
            pltpu.VMEM((2, 8, 256), f32),
            pltpu.VMEM((8, 512), f32),
            pltpu.VMEM((8, 512), f32),
            pltpu.VMEM((8, 8, 512), f32),
            pltpu.VMEM((8, 512), f32),
            pltpu.VMEM((4, 8, 512), f32),
            pltpu.VMEM((4, 8, 512), f32),
            dma((5,)),
            dma((9,)),
            dma((STEPS, 3)),
            dma((STEPS, 3)),
            dma((4,)),
            dma((4,)),
            dma((3, SLOTS)),
            dma((3, SLOTS)),
            dma((3, SLOTS)),
            dma((3, 3, 9)),
            dma((9,)),
            dma((9,)),
            dma((1,)),
            dma((1,)),
            dma((7,)),
            dma((8,)),
            dma((8,)),
            dma((8,)),
        ],
        compiler_params=pltpu.CompilerParams(
            collective_id=0, has_side_effects=True, vmem_limit_bytes=60 * 1024 * 1024
        ),
    )(hidden, hidden_check, down_weight, weight_check.T)
    out, rr, col = pl.pallas_call(hand_over, out_shape=shapes, in_specs=[vmem] * 3, out_specs=(vmem,) * 3)(*results)
    return out, rr.T, col.reshape(512)


def solution(mesh):
    placed = (P("dp", "tensor"), P(None, "tensor"), P("tensor", "dp"), P("tensor", "dp"))
    return jax.shard_map(
        shards,
        mesh=mesh,
        in_specs=placed,
        out_specs=(P("tensor", "dp"), P("tensor", "dp"), P("dp")),
        check_vma=False,
    )
```

```python
import jax
import jax.numpy as jnp
from jax import lax
from jax.experimental import pallas as pl
from jax.experimental.pallas import tpu as pltpu
from jax.sharding import PartitionSpec as P

CHECK_BLOCK = 128
MESH = pl.DeviceIdType.MESH

PIECE = 32
OWN = 8
STEPS = 19
AHEAD = 3
BLOCK = 64
SLOTS = 34


def kernel(
    h_hbm, hc_hbm, w_hbm, wc_hbm,
    out_hbm, rr_ref, col_ref,
    hbuf, wbuf, hcbuf, wcown, wcpar, wct, wck, pbuf, rbuf, zr, obuf, rrbuf, rrpart, rrt, rrpar, cbuf, colsum, nbuf, fbuf,
    lsem, osem, hs, hr, ws, wr, ds_s, ds_r, zs, zrs, os_s, os_r, fs, fr, cs, cr, vs, vr,
):
    f32, bf16 = jnp.float32, jnp.bfloat16
    dp = lax.axis_index("dp")
    t = lax.axis_index("tensor")
    x, y = dp // 4, dp % 4
    z, c = t // 2, t % 2
    group = y // 2
    role = (c + group) % 2
    x_next = ((x + 1) % 4) * 4 + y
    x_prev = ((x + 3) % 4) * 4 + y
    y_near = x * 4 + (y // 2) * 2 + (y + 1) % 2
    y_far = x * 4 + 3 - y
    t_other = z * 2 + 1 - c
    partner = (y_far, t_other)

    def remote(src, dst, send, recv, dev):
        return pltpu.make_async_remote_copy(
            src_ref=src, dst_ref=dst, send_sem=send, recv_sem=recv, device_id=dev, device_id_type=MESH
        )

    h_in = pltpu.make_async_copy(h_hbm, hbuf.at[pl.ds(0, PIECE * OWN)], lsem.at[0])
    w_in = [pltpu.make_async_copy(w_hbm.at[:, pl.ds(256 * j, 256)], wbuf.at[j], lsem.at[1 + j]) for j in range(2)]
    hc_in = pltpu.make_async_copy(hc_hbm, hcbuf, lsem.at[3])
    wc_in = pltpu.make_async_copy(wc_hbm, wcown, lsem.at[4])
    h_in.start()
    wc_in.start()
    w_in[0].start()
    w_in[1].start()
    hc_in.start()

    barrier = pltpu.get_barrier_semaphore()
    peers = [(x_next, t), (x_prev, t), (y_near, t)]
    peers += [(dp, (t + d) % 8) for d in range(1, 8)]
    peers += [(y_far, (t + d) % 8) for d in range(8)]
    for peer in peers:
        pl.semaphore_signal(barrier, inc=1, device_id=peer, device_id_type=MESH)
    pl.semaphore_wait(barrier, len(peers))

    def row_of(s, d):
        if s is None:
            return PIECE * d
        if s == STEPS - 1:
            return PIECE * (OWN + 54 + d)
        return PIECE * (OWN + 6 * (s // 2) + 2 * d + s % 2)

    def source(s, d):
        if s < 8:
            return None, s
        if d == 2:
            if s < 10:
                return 0, s - 8
            k = (0, 1, 4, 5, 2, 3, 6, 7)[s - 10]
            return 8 + k % 4, k // 4
        if s < 12:
            return (s - 8, 0) if d == 0 else (s - 4, 1)
        return s - 11, 2

    def dirs(s):
        return range(3) if s < STEPS - 1 else range(2)

    def h_copy(s, d):
        dev = ((x_next, t), (x_prev, t), (y_near, t))[d]
        return remote(
            hbuf.at[pl.ds(row_of(*source(s, d)), PIECE)],
            hbuf.at[pl.ds(row_of(s, d), PIECE)],
            hs.at[s, d],
            hr.at[s, d],
            dev,
        )

    h_in.wait()
    for s in range(AHEAD):
        for d in dirs(s):
            h_copy(s, d).start()
    wc_in.wait()
    wc_copy = remote(wcown, wcpar, ws.at[2], wr.at[2], (y_far, t))
    wc_copy.start()
    lows, highs = pl.ds(0, 128), pl.ds(128, 128)
    w_copy = [
        remote(wbuf.at[0], wbuf.at[2], ws.at[0], wr.at[0], (y_far, t)),
        remote(wbuf.at[1, :, lows], wbuf.at[3, :, lows], ws.at[1], wr.at[1], (y_far, t)),
        remote(wbuf.at[1, :, highs], wbuf.at[3, :, highs], ws.at[3], wr.at[3], (y_far, t)),
    ]
    for copy in w_in:
        copy.wait()
    for copy in w_copy:
        copy.start()

    both, first = (0, 2, 0, 256, 0), (0, 1, 0, 256, 0)
    third, fourth = (1, 1, 0, 128, 1), (1, 1, 128, 128, 2)

    def core_copy(half, slot, rows, j=0, lane=0, lanes=256):
        tag = half + lane // 128
        at = (slot, pl.ds(0, rows), pl.ds(lane, lanes))
        return remote(
            pbuf.at[(j,) + at], rbuf.at[(half,) + at], ds_s.at[tag, slot], ds_r.at[tag, slot], (dp, t_other)
        )

    def slot_of(pair, d):
        return 4 + 9 * d + pair

    def pair_slots(pair):
        if isinstance(pair, int) and pair == 4:
            return [(slot_of(4, 0), BLOCK), (slot_of(4, 1), BLOCK), (26, PIECE), (31, PIECE)]
        return [(slot_of(pair, d), BLOCK) for d in range(3)]

    own_slots = [(i, BLOCK) for i in range(4)]
    last_slots = [(32, PIECE), (33, PIECE)]

    def mm_part(row, slots, part):
        half, _, lane, lanes, _ = part
        m = sum(n for _, n in slots)
        out = jnp.dot(hbuf[pl.ds(row, m), :], wbuf[3, :, lane : lane + lanes], preferred_element_type=f32)
        at = 0
        for slot, n in slots:
            pbuf[3, slot, 0:n, lane : lane + lanes] = out[at : at + n]
            at += n

        @pl.when(role == 0)
        def _():
            for slot, n in slots:
                core_copy(1, slot, n, 3, lane, lanes).start()

    def mm(row, slots, j):
        m = sum(n for _, n in slots)
        out = jnp.dot(hbuf[pl.ds(row, m), :], wbuf[j], preferred_element_type=f32)
        at = 0
        for slot, n in slots:
            pbuf[j, slot, 0:n, :] = out[at : at + n]
            at += n
        for half in range(2):

            @pl.when(j == 2 * (1 - role) + half)
            def _():
                for slot, n in slots:
                    core_copy(half, slot, n + 8, j).start()

    def checks(row, slots):
        m = sum(n for _, n in slots)
        out = jnp.dot(hbuf[pl.ds(row, m), :], wck[...], preferred_element_type=f32)
        at = 0
        for slot, n in slots:
            turned = out[at : at + n].T
            pbuf[0, slot, n : n + 8, 0:n] = turned[0:8]
            pbuf[2, slot, n : n + 8, 0:n] = turned[16:24]
            at += n

    def compute(row, slots, n_j):
        checks(row, slots)

        @pl.loop(0, n_j)
        def _(i):
            j = (i + 2 * (1 - role)) % 4 if n_j == 4 else i
            mm(row, slots, j)

    def rows_of(item):
        return item[2] + (8 if item[0][0] == 0 else 0)

    def away(item):
        return (item[3] - z + 4) % 4

    def each(item):
        (h0, nh, lane, lanes, tag), (slot, ns), n, zd, q = item
        cols = slice(lane, lane + lanes)
        for half in range(h0, h0 + nh):
            for i in range(ns):
                yield half, slot + i, q + i, rows_of(item), cols

    def to_owner(r, item, side):
        (h0, nh, lane, lanes, tag), (slot, ns), n, zd, q = item
        tail = (pl.ds(0, rows_of(item)), pl.ds(lane, lanes))
        src = pbuf.at[(pl.ds(2 * r + h0, nh), pl.ds(slot, ns)) + tail]
        dst = zr.at[(1 + side, pl.ds(h0, nh), pl.ds(q, ns)) + tail]
        return remote(src, dst, zs.at[tag, slot], zrs.at[side, tag, q], (dp, zd * 2 + c))

    def add_up(r, item):
        lane, lanes = item[0][2:4]
        for half, slot, q, rows, cols in each(item):
            core_copy(half, slot, rows if lanes == 128 else item[2] + 8, 0, lane, lanes).wait_recv()

        @pl.when(away(item) == 0)
        def _():
            for half, slot, q, rows, cols in each(item):
                zr[0, half, q, 0:rows, cols] = pbuf[2 * r + half, slot, 0:rows, cols] + rbuf[half, slot, 0:rows, cols]

        @pl.when(away(item) != 0)
        def _():
            for half, slot, q, rows, cols in each(item):
                pbuf[2 * r + half, slot, 0:rows, cols] += rbuf[half, slot, 0:rows, cols]
            to_owner(r, item, away(item) - 1).start()

    def take(r, item):
        @pl.when(away(item) == 0)
        def _():
            for side in range(3):
                to_owner(r, item, side).wait_recv()

    def sent(r, item):
        @pl.when(away(item) != 0)
        def _():
            to_owner(r, item, 0).wait_send()

    def own_items(halves):
        def run(act):
            for i in (0, 2):
                act((halves, (i, 2), BLOCK, x, i))

        return run

    def early_items(halves, low, n):
        def run(act):
            @pl.loop(0, 3)
            def _(d):
                for pair in range(low, low + 4 if n == 2 else low + 1, n):
                    zd = (x + 3 - 2 * d + d // 2) % 4
                    act((halves, (slot_of(pair, d), n), BLOCK, zd, pair + 4 * (d // 2)))

        return run

    def late_items(halves, pair):
        def run(act):
            @pl.loop(0, 2)
            def _(d):
                if pair < 6:
                    act((halves, (slot_of(pair, d), 1), BLOCK, (x + 2) % 4, pair - 4 + 2 * d))
                else:
                    act((halves, (slot_of(pair, d), 1), BLOCK, (x + 3 - 2 * d + 4) % 4, pair - 1))

            if pair == 4:
                act((halves, (26, 1), PIECE, (x + 3) % 4, 4))
                act((halves, (31, 1), PIECE, (x + 1) % 4, 4))
            else:
                q = (4, 6, 5, 7)[pair - 5]
                act((halves, (slot_of(pair, 2), 1), BLOCK, (x + 2) % 4, q))

        return run

    def last_items(halves):
        def run(act):
            @pl.loop(0, 2)
            def _(d):
                act((halves, (32 + d, 1), PIECE, (x + 3 - 2 * d) % 4, 8))

        return run

    gone = [[], []]

    def over(r, items, act):
        @pl.when(role == r)
        def _():
            for run in items:
                run(lambda item: act(r, item))

    def collect(r, items, pair=0):
        over(r, items, add_up)
        gone[r] += [(run, pair) for run in items]

    wct[...] = jnp.zeros_like(wct)
    wct[0:4, :] = wcown[...]
    wc_copy.wait_recv()
    wct[16:20, :] = wcpar[...]

    @pl.loop(0, wct.shape[1] // 128)
    def _(i):
        part = pl.ds(pl.multiple_of(i * 128, 128), 128)
        wck[part, :] = wct[:, part].astype(f32).T.astype(bf16)

    compute(0, own_slots, 2)
    collect(0, [own_items(both)])

    hc_in.wait()
    for half in range(2):
        rows = jnp.dot(hcbuf[...], wbuf[half], preferred_element_type=f32)
        cbuf[t, :, 256 * half : 256 * (half + 1)] = rows[0:8] + rows[8:16]
    check_copies = [
        remote(cbuf.at[t], cbuf.at[t], cs.at[d - 1], cr.at[t], (dp, (t + d) % 8)) for d in range(1, 8)
    ]
    for copy in check_copies:
        copy.start()
    colsum[...] = jnp.zeros_like(colsum)

    def arrive(s):
        for d in dirs(s):
            h_copy(s, d).wait_recv()
        for later in range(AHEAD, STEPS):
            for d in dirs(later):
                if max(later - AHEAD, source(later, d)[0] or 0) == s:
                    h_copy(later, d).start()

    def out_copies(q, row, n):
        rows = pl.ds(pl.multiple_of(row, PIECE), n)
        near = pltpu.make_async_copy(obuf.at[rows], out_hbm.at[rows], osem.at[q])
        far = remote(obuf.at[rows], out_hbm.at[rows], os_s.at[q], os_r.at[q], partner)
        return near, far

    def finish(q, row, n):
        lane = lax.broadcasted_iota(jnp.int32, (n, 128), 1)
        marks = jnp.zeros((n, 128), f32)
        for half in range(2):
            full = (zr[0, half, q, 0:n, :] + zr[1, half, q, 0:n, :]) + (zr[2, half, q, 0:n, :] + zr[3, half, q, 0:n, :])
            obuf[pl.ds(pl.multiple_of(row, PIECE), n), 256 * half : 256 * (half + 1)] = full.astype(bf16)
            colsum[:, 256 * half : 256 * (half + 1)] += full.reshape(n // 8, 8, 256).sum(0)
            for b in range(2):
                sums = full[:, 128 * b : 128 * (b + 1)].sum(-1, keepdims=True)
                marks = jnp.where(lane == 2 * half + b, sums, marks)
        near, far = out_copies(q, row, n)

        @pl.when(role == 0)
        def _():
            near.start()

        @pl.when(role == 1)
        def _():
            far.start()

        check = (zr[0, 0, q, n : n + 8, 0:n] + zr[1, 0, q, n : n + 8, 0:n]) + (
            zr[2, 0, q, n : n + 8, 0:n] + zr[3, 0, q, n : n + 8, 0:n]
        )
        rrbuf[q, :, 0:n] = (check - marks.T[0:8]) * CHECK_BLOCK ** (-0.5)

    row_own = (y % 2) * 256
    row_near = ((y + 1) % 2) * 256
    apart = (z - x + 4) % 2

    def finish_near(act, late):
        @pl.when(apart == 0)
        def _():
            @pl.loop(7 if late else 4, 8 if late else 7)
            def _(q):
                act(q, row_near + BLOCK * (q - 4), BLOCK)

        @pl.when(apart == 1)
        def _():
            act(8 if late else 4, row_near + (224 if late else 0), PIECE)

            @pl.loop(7 if late else 5, 8 if late else 7)
            def _(q):
                act(q, row_near + PIECE + BLOCK * (q - 5), BLOCK)

    def finish_own(act):
        @pl.loop(0, 4)
        def _(q):
            act(q, row_own + BLOCK * q, BLOCK)

    def early_mm(one):
        one(0, own_slots)

        @pl.loop(0, 4)
        def _(pair):
            one(PIECE * OWN + 192 * pair, pair_slots(pair))

    def late_mm(one, low, high):
        for pair in range(low, min(high, 5)):
            one(row_of(2 * pair, 0), pair_slots(pair))
        if high > 5:

            @pl.loop(max(low, 5), high)
            def _(pair):
                one(PIECE * OWN + 192 * pair, pair_slots(pair))

    for pair in range(9):
        arrive(2 * pair)
        arrive(2 * pair + 1)
        row, slots = row_of(2 * pair, 0), pair_slots(pair)
        compute(row, slots, 2 if pair < 4 else 3 if pair < 8 else 4)
        if pair < 4:
            collect(0, [early_items(both, pair, 1)])
        else:
            collect(0, [late_items(both, pair)], pair)
            collect(1, [late_items(first if pair < 8 else both, pair)], pair)
        if pair == 3:
            w_copy[0].wait_recv()
            early_mm(lambda row, slots: mm(row, slots, 2))
            collect(1, [own_items(first), early_items(first, 0, 2)])
        for at, part in ((5, third), (7, fourth)):
            if pair == at:
                w_copy[part[-1]].wait_recv()
                early_mm(lambda row, slots: mm_part(row, slots, part))
                collect(1, [own_items(part), early_items(part, 0, 2)])
                late_mm(lambda row, slots: mm_part(row, slots, part), 4, pair + 1)
                collect(1, [late_items(part, k) for k in range(4, pair + 1)])
            elif at < pair < 8 and part == third:
                mm_part(row, slots, part)
                collect(1, [late_items(part, pair)])
    early_gone = [[run for run, pair in gone[r] if pair < 8] for r in range(2)]
    late_gone = [[run for run, pair in gone[r] if pair == 8] for r in range(2)]

    arrive(18)
    compute(row_of(18, 0), last_slots, 4)
    for r in range(2):
        collect(r, [last_items(both)], 8)
        late_gone[r].append(last_items(both))
    for r in range(2):
        over(r, early_gone[r], take)
    finish_own(finish)
    finish_near(finish, False)
    for r in range(2):
        over(r, late_gone[r], take)
    finish_near(finish, True)

    near_copies = [remote(colsum, nbuf.at[z], vs.at[d], vr.at[z], (dp, (t + d) % 8)) for d in range(1, 8)]
    far_copies = [remote(colsum, fbuf.at[z], vs.at[d], vr.at[4 + z], (y_far, (t + d) % 8)) for d in range(8)]
    rr_far = remote(rrt, rrpar, fs.at[0], fr.at[0], partner)

    @pl.when(role == 0)
    def _():
        for copy in near_copies:
            copy.start()
        nbuf[z] = colsum[...]

    @pl.when(role == 1)
    def _():
        for copy in far_copies:
            copy.start()

    for q in range(4):
        rrpart[0, :, BLOCK * q : BLOCK * (q + 1)] = rrbuf[q, :, 0:BLOCK]

    @pl.when(apart == 0)
    def _():
        for q in range(4):
            rrpart[1, :, BLOCK * q : BLOCK * (q + 1)] = rrbuf[4 + q, :, 0:BLOCK]

    @pl.when(apart == 1)
    def _():
        rrpart[1, :, 0:PIECE] = rrbuf[4, :, 0:PIECE]
        for q in range(3):
            rrpart[1, :, PIECE + BLOCK * q : PIECE + BLOCK * (q + 1)] = rrbuf[5 + q, :, 0:BLOCK]
        rrpart[1, :, 256 - PIECE : 256] = rrbuf[8, :, 0:PIECE]

    rrt[:, pl.ds(pl.multiple_of(row_own, 256), 256)] = rrpart[0]
    rrt[:, pl.ds(pl.multiple_of(row_near, 256), 256)] = rrpart[1]

    @pl.when(role == 0)
    def _():
        rr_ref[...] = rrt[0:4]

    @pl.when(role == 1)
    def _():
        rr_far.start()

    for s in range(STEPS):
        for d in dirs(s):
            h_copy(s, d).wait_send()
    wc_copy.wait_send()
    for copy in w_copy:
        copy.wait_send()
    for copy in check_copies:
        copy.wait_send()
    def given(slot, n, split=True):
        core_copy(0, slot, n + 8).wait_send()
        if not split:
            core_copy(1, slot, n + 8).wait_send()
            return

        @pl.when(role == 1)
        def _():
            core_copy(1, slot, n + 8).wait_send()

        @pl.when(role == 0)
        def _():
            for part in (third, fourth):
                core_copy(1, slot, n, 3, part[2], part[3]).wait_send()

    for low, high in ((0, 12), (13, 21), (22, 26), (27, 30)):

        @pl.loop(low, high)
        def _(slot):
            given(slot, BLOCK)

    for slot in (12, 21, 30):
        given(slot, BLOCK, False)
    for slot in (26, 31):
        given(slot, PIECE)
    for slot in (32, 33):
        given(slot, PIECE, False)
    for r in range(2):
        over(r, early_gone[r] + late_gone[r], sent)

    def written(side):
        def act(q, row, n):
            out_copies(q, row, n)[side].wait()

        finish_own(act)
        for late in (False, True):
            finish_near(act, late)

    total = cbuf[t]
    for d in range(1, 8):
        src = (t + d) % 8
        remote(cbuf.at[src], cbuf.at[src], cs.at[d - 1], cr.at[src], (dp, src)).wait_recv()
        total = total + cbuf[src]

    @pl.when(role == 0)
    def _():
        for d in range(1, 4):
            src = (z + d) % 4
            remote(colsum, nbuf.at[src], vs.at[0], vr.at[src], (dp, t_other)).wait_recv()

    @pl.when(role == 1)
    def _():
        for src in range(4):
            remote(colsum, nbuf.at[src], vs.at[0], vr.at[src], (dp, t_other)).wait_recv()

    for src in range(4):
        remote(colsum, fbuf.at[src], vs.at[0], vr.at[4 + src], partner).wait_recv()
    sums = (nbuf[0] + nbuf[1]) + (nbuf[2] + nbuf[3])
    sums = sums + ((fbuf[0] + fbuf[1]) + (fbuf[2] + fbuf[3]))
    col_ref[...] = (total - sums).sum(0, keepdims=True) * 4096 ** (-0.5)

    @pl.when(role == 0)
    def _():
        written(0)

        for copy in near_copies:
            copy.wait_send()

    @pl.when(role == 1)
    def _():
        rr_far.wait()
        rr_ref[...] = rrpar[0:4]

        written(1)

        for copy in far_copies:
            copy.wait_send()


def hand_over(out_in, rr_in, col_in, out_ref, rr_ref, col_ref):
    out_ref[...] = out_in[...]
    rr_ref[...] = rr_in[...]
    col_ref[...] = col_in[...]


def shards(hidden, hidden_check, down_weight, weight_check):
    f32, bf16 = jnp.float32, jnp.bfloat16
    k = hidden.shape[1]
    dma = pltpu.SemaphoreType.DMA
    shapes = (
        jax.ShapeDtypeStruct((512, 512), bf16),
        jax.ShapeDtypeStruct((4, 512), f32),
        jax.ShapeDtypeStruct((1, 512), f32),
    )
    vmem = pl.BlockSpec(memory_space=pltpu.VMEM)
    whole = pl.BlockSpec(memory_space=pl.ANY)
    results = pl.pallas_call(
        kernel,
        out_shape=shapes,
        in_specs=[whole] * 4,
        out_specs=(whole, vmem, vmem),
        scratch_shapes=[
            pltpu.VMEM((2048, k), bf16),
            pltpu.VMEM((4, k, 256), bf16),
            pltpu.VMEM((16, k), bf16),
            pltpu.VMEM((4, k), bf16),
            pltpu.VMEM((4, k), bf16),
            pltpu.VMEM((128, k), bf16),
            pltpu.VMEM((k, 128), bf16),
            pltpu.VMEM((4, SLOTS, BLOCK + 8, 256), f32),
            pltpu.VMEM((2, SLOTS, BLOCK + 8, 256), f32),
            pltpu.VMEM((4, 2, 9, BLOCK + 8, 256), f32),
            pltpu.VMEM((512, 512), bf16),
            pltpu.VMEM((9, 8, 128), f32),
            pltpu.VMEM((2, 8, 256), f32),
            pltpu.VMEM((8, 512), f32),
            pltpu.VMEM((8, 512), f32),
            pltpu.VMEM((8, 8, 512), f32),
            pltpu.VMEM((8, 512), f32),
            pltpu.VMEM((4, 8, 512), f32),
            pltpu.VMEM((4, 8, 512), f32),
            dma((5,)),
            dma((9,)),
            dma((STEPS, 3)),
            dma((STEPS, 3)),
            dma((4,)),
            dma((4,)),
            dma((3, SLOTS)),
            dma((3, SLOTS)),
            dma((3, SLOTS)),
            dma((3, 3, 9)),
            dma((9,)),
            dma((9,)),
            dma((1,)),
            dma((1,)),
            dma((7,)),
            dma((8,)),
            dma((8,)),
            dma((8,)),
        ],
        compiler_params=pltpu.CompilerParams(
            collective_id=0, has_side_effects=True, vmem_limit_bytes=60 * 1024 * 1024
        ),
    )(hidden, hidden_check, down_weight, weight_check.T)
    out, rr, col = pl.pallas_call(hand_over, out_shape=shapes, in_specs=[vmem] * 3, out_specs=(vmem,) * 3)(*results)
    return out, rr.T, col.reshape(512)


def solution(mesh):
    placed = (P("dp", "tensor"), P(None, "tensor"), P("tensor", "dp"), P("tensor", "dp"))
    return jax.shard_map(
        shards,
        mesh=mesh,
        in_specs=placed,
        out_specs=(P("tensor", "dp"), P("tensor", "dp"), P("dp")),
        check_vma=False,
    )
```
